32 devices in a mesh: grp: 8 (over z, x), dom: 4 (over y, core).
Axes of the slice: x: 2, y: 2, z: 4, core: 2. Of those that a mesh axis runs over, the one named last changes fastest.
Arguments:
- positions: float32 [3, 4096, 512], P(None, ('grp', 'dom')), may hold values from 0 to 1
- velocities: float32 [3, 4096, 512], P(None, ('grp', 'dom')), may hold values from -6 to 6
- masses: float32 [4096, 512], P(('grp', 'dom')), may hold values from 0.5 to 2
- block_halo: int32 [4096], P(('grp', 'dom')), may hold values from 0 to 4095, as said below
- block_shift: int32 [3, 4096], P(None, ('grp', 'dom')), may hold values from -1 to 1
- block_live: int32 [4096], P(('grp', 'dom')), may hold values from 64 to 512
- block_count: int32 [32], P(('grp', 'dom')), may hold values from 32 to 128
- home_slot: int32 [4096], replicated, may hold values from 0 to 4095, as said below
Outputs:
- halo_table: float32 [11, 4096], P(None, ('grp', 'dom'))
- kinetic: float32 [4096, 512], P(('grp', 'dom'))
- radial: float32 [4096, 512], P(('grp', 'dom'))
The draws below stay inside these ranges and needn't reach their ends.
Inputs may be any that keep to these rules, and one draw needn't show every extreme that they name: A permutation: the halo h is owned by the device of index home_slot[h] // 128 (grp+dom order), in its column home_slot[h] % 128. `block_halo`: the owner of a block's halo lies in the block's own index of grp or in the next one (index + 1, wrapping around); both occur.
All inputs are finite; a program needn't handle non-finite values.
Results may differ from the reference program's by a relative error of at most 0.0003.
Values sent between devices are 32-bit elements; how exact they have to be, the bound alone decides.
A program may use at most 64 MiB of HBM per device.

```python
import math
import jax
import jax.numpy as jnp
from jax import lax

BS = 512
BLK_DEV = 128
HALO_DEV = 128
NB = 4096
HALOS = 4096
N_GRP = 8
N_DOM = 4
DEVICES = 32


def owner_table(key):
    return jax.random.permutation(jax.random.fold_in(key, 11), HALOS).astype(jnp.int32)


def draw_home_slot(key, part):
    return owner_table(key)


def draw_block_halo(key, part):
    home = owner_table(key)
    inverse = jnp.argsort(home).astype(jnp.int32)
    window = N_DOM * HALO_DEV
    first_key, second_key, third_key = jax.random.split(jax.random.fold_in(key, 23), 3)
    limit = jax.random.randint(first_key, (NB,), 1, 2 * window + 1)
    picked = jax.random.randint(second_key, (NB,), 0, limit)
    mixing = jax.random.permutation(third_key, 2 * window).astype(jnp.int32)
    picked = mixing[picked]
    group_index = jnp.arange(NB, dtype=jnp.int32) // BLK_DEV // N_DOM
    column = (group_index + picked // window) % N_GRP * window + picked % window
    return inverse[column].astype(jnp.int32)


def touch_ends(values, rng, least, top_value):
    extent = values.shape
    spot = [jax.random.randint(jax.random.fold_in(rng, axis), (), 0, extent[axis]) for axis in range(len(extent))]
    values = values.at[tuple(spot)].set(least)
    longest = extent.index(max(extent))
    spot[longest] = (spot[longest] + 1) % extent[longest]
    return values.at[tuple(spot)].set(top_value)


def steps_of(rng, dims, cuts, smallest, top_value):
    level = 1.0
    for axis_at, shards_of in cuts:
        draws = jax.random.uniform(jax.random.fold_in(jax.random.fold_in(rng, 6), axis_at), (shards_of,), jnp.float32, smallest / len(cuts), top_value / len(cuts))
        level = level * jnp.repeat(jnp.exp(draws), dims[axis_at] // shards_of).reshape((-1,) + (1,) * (len(dims) - 1 - axis_at))
    return level


def normal_values(own_key, extent, scale, bound, pieces=(), kind=jnp.bfloat16):
    entries = scale * jax.random.normal(own_key, extent, jnp.float32)
    if pieces:
        entries = entries * steps_of(own_key, extent, pieces, -0.22, 0.18)
    return jnp.clip(entries, -bound, bound).astype(kind)


def setup_inputs(seed: int = 0) -> dict:
    key_of = jax.random.split(jax.random.key(seed), 9)
    positions = jnp.clip(1.0 * jax.random.uniform(key_of[0], (3, NB, BS), jnp.float32) ** steps_of(key_of[0], (3, NB, BS), ((1, 32),), -0.2, 0.2), 0.0, 1.0)
    velocities = normal_values(key_of[1], (3, NB, BS), 1.0, 6.0, ((1, 32),), jnp.float32)
    masses = jnp.clip(jnp.exp(math.log(2.0) - 1.3862944 * jax.random.uniform(key_of[2], (NB, BS), jnp.float32) ** steps_of(key_of[2], (NB, BS), ((0, 32),), -0.2, 0.2)), 0.5, 2.0)
    block_halo = draw_block_halo(jax.random.fold_in(key_of[8], 71), 0)
    block_shift = touch_ends(jax.random.randint(key_of[4], (3, NB), -1, 2), jax.random.fold_in(key_of[4], 1), -1, 1).astype(jnp.int32)
    block_live = touch_ends(jax.random.randint(key_of[5], (NB,), BS // 8, BS + 1), jax.random.fold_in(key_of[5], 1), BS // 8, BS).astype(jnp.int32)
    block_count = touch_ends(jax.random.randint(key_of[6], (DEVICES,), max(1, BLK_DEV // 4), BLK_DEV + 1), jax.random.fold_in(key_of[6], 1), max(1, BLK_DEV // 4), BLK_DEV).astype(jnp.int32)
    home_slot = draw_home_slot(jax.random.fold_in(key_of[8], 71), 0)
    return {"positions": positions, "velocities": velocities, "masses": masses, "block_halo": block_halo, "block_shift": block_shift, "block_live": block_live, "block_count": block_count, "home_slot": home_slot}


BOX = 1.0
EPSILON = 1e-6


def crossed(first, second):
    return jnp.stack([first[1] * second[2] - first[2] * second[1],
                      first[2] * second[0] - first[0] * second[2],
                      first[0] * second[1] - first[1] * second[0]])


def block_moments(positions, velocities, masses, block_shift, block_live, valid):
    lanes = jnp.arange(masses.shape[1], dtype=jnp.int32)
    live_mask = ((lanes[None, :] < block_live[:, None]) & valid[:, None]).astype(masses.dtype)
    weights = masses * live_mask
    unwrapped = positions + BOX * block_shift.astype(positions.dtype)[:, :, None]
    speed_sq = jnp.sum(velocities * velocities, axis=0)
    angular = crossed(unwrapped, velocities)
    rows = [jnp.sum(weights, axis=1)[None], jnp.sum(weights * unwrapped, axis=2),
            jnp.sum(weights * velocities, axis=2), jnp.sum(weights * speed_sq, axis=1)[None],
            jnp.sum(weights * angular, axis=2)]
    return jnp.concatenate(rows, axis=0), live_mask, unwrapped


def halo_properties(sums, total, halos):
    heavy = jnp.maximum(sums[0], 1.0)
    centre = sums[1:4] / heavy
    drift = sums[4:7] / heavy
    spread = sums[7] / heavy - jnp.sum(drift * drift, axis=0)
    spin = sums[8:11] / heavy - crossed(centre, drift)
    share = sums[0] * halos / total
    return jnp.concatenate([share[None], centre, drift, spread[None], spin], axis=0)


def particle_outputs(unwrapped, velocities, live_mask, stats):
    centre = stats[0:3][:, :, None]
    drift = stats[3:6][:, :, None]
    spread = stats[6][:, None]
    offset = velocities - drift
    kinetic = jnp.sum(offset * offset, axis=0) / (3.0 * spread + EPSILON)
    distance = unwrapped - centre
    radial = jnp.sum(distance * distance, axis=0)
    return kinetic * live_mask, radial * live_mask


def reference(positions, velocities, masses, block_halo, block_shift, block_live, block_count, home_slot):
    groups = block_count.shape[0]
    total_blocks = masses.shape[0]
    width = masses.shape[1]
    grouped_pos = positions.reshape(3, groups, BLK_DEV, width).transpose(1, 0, 2, 3)
    grouped_vel = velocities.reshape(3, groups, BLK_DEV, width).transpose(1, 0, 2, 3)
    grouped_mass = masses.reshape(groups, BLK_DEV, width)
    grouped_shift = block_shift.reshape(3, groups, BLK_DEV).transpose(1, 0, 2)
    grouped_live = block_live.reshape(groups, BLK_DEV)
    valid = jnp.arange(BLK_DEV, dtype=jnp.int32)[None, :] < block_count[:, None]

    def per_group(items):
        place, speed, weight, shift, alive, usable = items
        return block_moments(place, speed, weight, shift, alive, usable)[0]

    moments = lax.map(per_group, (grouped_pos, grouped_vel, grouped_mass, grouped_shift, grouped_live, valid))
    moments = moments.transpose(1, 0, 2).reshape(11, total_blocks)
    slots = home_slot[block_halo]
    halos = home_slot.shape[0]
    sums = jnp.zeros((11, halos), moments.dtype).at[:, slots].add(moments)
    total = jnp.sum(moments[0])
    halo_table = halo_properties(sums, total, halos)
    stats = halo_table[1:8][:, slots].reshape(7, groups, BLK_DEV).transpose(1, 0, 2)

    def outputs(items):
        place, speed, weight, shift, alive, usable, local_stats = items
        _, live_mask, unwrapped = block_moments(place, speed, weight, shift, alive, usable)
        return particle_outputs(unwrapped, speed, live_mask, local_stats)

    kinetic, radial = lax.map(outputs, (grouped_pos, grouped_vel, grouped_mass, grouped_shift, grouped_live, valid, stats))
    return halo_table, kinetic.reshape(total_blocks, width), radial.reshape(total_blocks, width)
```

```python
import functools

import jax
import jax.numpy as jnp
from jax import lax
from jax.experimental import pallas as pl
from jax.experimental.pallas import tpu as pltpu
from jax.sharding import PartitionSpec as P

BOX = 1.0
EPSILON = 1e-06
MESH = pl.DeviceIdType.MESH
F32 = jnp.float32
BF16 = jnp.bfloat16
LANES = 128
CHUNKS = 4
SLOT_ROW = 8
SPIN_ROW = 9
USED_ROWS = 12
MASS_ROW = 12


def pieces(x):
    hi = x.astype(BF16).astype(F32)
    rest = x - hi
    mid = rest.astype(BF16).astype(F32)
    return hi, mid, rest - mid


def quotient(x, n):
    return x >> (n.bit_length() - 1) if n & (n - 1) == 0 else x // n


def crossed(a, b):
    return (a[1] * b[2] - a[2] * b[1], a[2] * b[0] - a[0] * b[2], a[0] * b[1] - a[1] * b[0])


def exchange_kernel(
    groups, domains, owned,
    pos_hbm, vel_hbm, mass_hbm, halo_hbm, shift_hbm, live_hbm, count_hbm, home_hbm,
    pos, vel, means_ref, sums_ref,
    halo_ref, shift_ref, live_ref, count_ref, home_ref, mass, cols, slots, moments, tile, mass_row, near_in, far_in,
    small_sem, in_sem, send_near, recv_near, send_far, recv_far,
):
    blocks, width = mass.shape
    rows = blocks // CHUNKS
    g = lax.axis_index("grp")
    d = lax.axis_index("dom")

    def wrapped(x, n):
        return jnp.where(x >= n, x - n, x)

    def peer(dg, dd):
        return {"grp": wrapped(g + dg % groups, groups), "dom": wrapped(d + dd % domains, domains)}

    pairs = (
        (live_hbm, live_ref), (count_hbm, count_ref), (halo_hbm, halo_ref), (home_hbm, home_ref),
        (shift_hbm, shift_ref),
    )
    smalls = [
        pltpu.make_async_copy(src, dst, small_sem.at[k]) for k, (src, dst) in enumerate(pairs)
    ]
    for copy in smalls:
        copy.start()
    loads = []
    for c in range(CHUNKS):
        part = pl.ds(c * rows, rows)
        group = [
            pltpu.make_async_copy(mass_hbm.at[part], mass.at[part], in_sem.at[3 * c]),
            pltpu.make_async_copy(pos_hbm.at[:, part], pos.at[:, part], in_sem.at[3 * c + 1]),
            pltpu.make_async_copy(vel_hbm.at[:, part], vel.at[:, part], in_sem.at[3 * c + 2]),
        ]
        for n, copy in enumerate(group):
            copy.start(priority=(c + n) % 2)
        loads.append(group)

    ahead = [(1, dd) for dd in range(domains)]
    behind = [(groups - 1, dd) for dd in range(domains)]
    inside = [(0, dd) for dd in range(1, domains)]
    far = [(dg, dd) for dg in range(2, groups - 1) for dd in range(domains)]
    near = ahead + behind + inside
    barrier = pltpu.get_barrier_semaphore()
    for dg, dd in near + far:
        pl.semaphore_signal(barrier, inc=1, device_id=peer(dg, dd), device_id_type=MESH)

    for copy in smalls:
        copy.wait()

    lane = lax.broadcasted_iota(jnp.int32, (blocks, LANES), 1)
    row = lax.broadcasted_iota(jnp.int32, (blocks, 1), 0)
    packed = jnp.concatenate(
        [
            halo_ref[...].astype(F32),
            live_ref[...].astype(F32),
            jnp.zeros((LANES - 2, blocks), F32),
        ],
        axis=0,
    )
    turned = packed.T
    cols[...] = jnp.where(row < count_ref[0, 0], turned[:, 1:2], 0.0)

    halo = turned[:, 0:1].astype(jnp.int32)
    home = home_ref[...]
    home_rows = home.shape[0]
    row_pick = lax.broadcasted_iota(jnp.int32, (blocks, home_rows), 1) == quotient(halo, LANES)
    split = jnp.concatenate([(home >> 8).astype(F32), (home & 255).astype(F32)], axis=1)
    picked = jnp.dot(
        row_pick.astype(F32).astype(BF16), split.astype(BF16), preferred_element_type=F32
    )
    value = picked[:, :LANES] * 256.0 + picked[:, LANES:]
    slot = jnp.sum(jnp.where(lane == (halo & (LANES - 1)), value, 0.0), axis=1, keepdims=True)
    slots[...] = jnp.broadcast_to(slot, (blocks, LANES))

    lane8 = lax.broadcasted_iota(jnp.int32, (8, LANES), 1)
    shift = shift_ref[...].astype(F32) * BOX

    def moment_rows(start):
        at = pl.ds(start, 8)
        live = jnp.broadcast_to(cols[at], (8, LANES))
        sums = None
        for t in range(width // LANES):
            span = pl.ds(t * LANES, LANES)
            place = (lane8 + t * LANES).astype(F32)
            w = jnp.where(place < live, mass[at, span], 0.0)
            x = [pos[k, at, span] for k in range(3)]
            v = [vel[k, at, span] for k in range(3)]
            wv = [w * y for y in v]
            made = [w] + [w * y for y in x] + wv
            made += [wv[0] * v[0] + wv[1] * v[1] + wv[2] * v[2]]
            made += list(crossed(x, wv))
            sums = made if sums is None else [a + b for a, b in zip(sums, made)]
        out = jnp.where(lane8 == SLOT_ROW, slots[at], 0.0)
        for k, y in enumerate(sums):
            lane_at = k if k < SLOT_ROW else k + 1
            out = jnp.where(lane8 == lane_at, jnp.sum(y, axis=1, keepdims=True), out)
        moments[at] = out

    for c in range(CHUNKS):
        for copy in loads[c]:
            copy.wait()

        def step(i, carry, c=c):
            moment_rows(pl.multiple_of(c * rows + i * 8, 8))
            return carry

        lax.fori_loop(0, rows // 8, step, 0, unroll=True)

    by_row = moments[...].T[:16]
    blank = jnp.zeros((1, blocks), F32)
    s = [shift[k:k + 1] for k in range(3)]
    v = [by_row[4 + k:5 + k] for k in range(3)]

    def stack(x, first):
        return jnp.concatenate([blank] * first + list(x) + [blank] * (5 - first), axis=0)

    first = by_row[0:8] + stack(s, 1) * by_row[0:1]
    turn = stack((s[1], s[2], s[0]), 1) * stack((v[2], v[0], v[1]), 1)
    turn = turn - stack((s[2], s[0], s[1]), 1) * stack((v[1], v[2], v[0]), 1)
    second = by_row[8:16] + turn
    tile[0:8] = first
    tile[8:16] = second
    mass_row[0] = first[0:1]

    pl.semaphore_wait(barrier, len(near) + len(far))

    def near_copy(k, dg, dd):
        part = pl.ds(0, SLOT_ROW + 1) if dg == groups - 1 else pl.ds(0, USED_ROWS)
        return pltpu.make_async_remote_copy(
            src_ref=tile.at[part], dst_ref=near_in.at[k, part],
            send_sem=send_near.at[k], recv_sem=recv_near.at[k],
            device_id=peer(dg, dd), device_id_type=MESH,
        )

    def far_copy(k, dg, dd):
        return pltpu.make_async_remote_copy(
            src_ref=mass_row.at[0], dst_ref=far_in.at[pl.ds(k, 1)],
            send_sem=send_far.at[k], recv_sem=recv_far.at[k],
            device_id=peer(dg, dd), device_id_type=MESH,
        )

    near_copies = [near_copy(k, *p) for k, p in enumerate(near)]
    far_copies = [far_copy(k, *p) for k, p in enumerate(far)]
    from_behind = range(0, domains)
    from_ahead = range(domains, 2 * domains)
    from_inside = range(2 * domains, len(near))
    for copy in near_copies[:2 * domains] + far_copies + near_copies[2 * domains:]:
        copy.start()

    row8 = lax.broadcasted_iota(jnp.int32, (8, blocks), 0)
    base = ((g * domains + d) * owned).astype(F32)
    mine = lax.broadcasted_iota(jnp.int32, (owned, blocks), 0).astype(F32) + base

    def gather(tiles, own):
        left, right = [], []
        for upper, lower in tiles:
            place = lower[0:1]
            hit = (slots[...] == place).astype(F32)
            if own:
                body = jnp.concatenate([upper, jnp.where(row8 < USED_ROWS - 8, lower, 0.0)], axis=0)
                hit = jnp.concatenate([hit, (mine == place).astype(F32)], axis=0)
                left.append(jnp.concatenate(pieces(body), axis=0))
            else:
                left.append(jnp.concatenate(list(pieces(upper)) + [jnp.zeros_like(upper)], axis=0))
            right.append(hit)
        left = jnp.concatenate(left, axis=1).astype(BF16)
        right = jnp.concatenate(right, axis=1).astype(BF16)
        out = lax.dot_general(left, right, (((1,), (1,)), ((), ())), preferred_element_type=F32)
        n = 16 if own else 8
        return out[0:n] + out[n:2 * n] + out[2 * n:3 * n]

    def inbox(ks):
        for k in ks:
            near_copies[k].wait_recv()
        return [(near_in[k, 0:8], near_in[k, 8:16]) for k in ks]

    total = first[0:1]
    tiles = inbox(from_inside)
    total = functools.reduce(lambda a, b: a + b, [t[0][0:1] for t in tiles], total)
    held = gather([(first, second)] + tiles, True)
    means, sums = held[0:8, :blocks], held[:, blocks:]
    tiles = inbox(from_ahead)
    total = functools.reduce(lambda a, b: a + b, [t[0][0:1] for t in tiles], total)
    means = means + gather(tiles, False)
    for copy in near_copies + far_copies:
        copy.wait_send()
    tiles = inbox(from_behind)
    total = functools.reduce(lambda a, b: a + b, [t[0][0:1] for t in tiles], total)
    held = gather(tiles, True)
    means = means + held[0:8, :blocks]
    sums = sums + held[:, blocks:]

    centre, drift, spread = halo_means(means)
    live = jnp.where(
        lax.broadcasted_iota(jnp.int32, (1, blocks), 1) < count_ref[0, 0],
        live_ref[...].astype(F32), 0.0,
    )
    by_block = jnp.concatenate(
        [centre[k] - s[k] for k in range(3)]
        + drift
        + [1.0 / (3.0 * spread + EPSILON), live, jnp.zeros((LANES - 8, blocks), F32)],
        axis=0,
    )
    means_ref[...] = by_block.T

    for copy in far_copies:
        copy.wait_recv()
    if far_copies:
        total = total + jnp.sum(far_in[...], axis=0, keepdims=True)
    sums_ref[0:8] = sums[0:8]
    sums_ref[8:16] = jnp.where(row8 == MASS_ROW - 8, total, sums[8:16])


def halo_means(sums):
    scaled = sums[1:8] * (1.0 / jnp.maximum(sums[0:1], 1.0))
    centre = [scaled[k:k + 1] for k in range(3)]
    drift = [scaled[3 + k:4 + k] for k in range(3)]
    spread = scaled[6:7] - (drift[0] * drift[0] + drift[1] * drift[1] + drift[2] * drift[2])
    return centre, drift, spread


def output_kernel(
    halos, pos, vel, means_ref, sums_ref, table_hbm, kin_hbm, rad_hbm, table, kin, rad, sem
):
    blocks, width = kin.shape
    rows = blocks // CHUNKS
    position8 = lax.broadcasted_iota(jnp.int32, (8, width), 1).astype(F32)

    sums = sums_ref[...]
    centre, drift, spread = halo_means(sums)
    heavy_inv = 1.0 / jnp.maximum(sums[0:1], 1.0)
    turned_spin = crossed(centre, drift)
    spin = [sums[SPIN_ROW + k:SPIN_ROW + 1 + k] * heavy_inv - turned_spin[k] for k in range(3)]
    total = jnp.sum(sums[MASS_ROW:MASS_ROW + 1], axis=1, keepdims=True)
    share = sums[0:1] * float(halos) / total
    table[...] = jnp.concatenate([share] + centre + drift + [spread] + spin, axis=0)
    stores = [pltpu.make_async_copy(table, table_hbm, sem.at[2 * CHUNKS])]
    stores[0].start()

    def output_rows(start):
        at = pl.ds(start, 8)
        mean = means_ref[at]
        live = position8 < mean[:, 7:8]
        kinetic = 0.0
        radial = 0.0
        for k in range(3):
            distance = pos[k, at] - mean[:, k:k + 1]
            radial = radial + distance * distance
            offset = vel[k, at] - mean[:, 3 + k:4 + k]
            kinetic = kinetic + offset * offset
        kin[at] = jnp.where(live, kinetic * mean[:, 6:7], 0.0)
        rad[at] = jnp.where(live, radial, 0.0)

    for c in range(CHUNKS):

        def step(i, carry, c=c):
            output_rows(pl.multiple_of(c * rows + i * 8, 8))
            return carry

        lax.fori_loop(0, rows // 8, step, 0, unroll=True)
        part = pl.ds(c * rows, rows)
        group = [
            pltpu.make_async_copy(kin.at[part], kin_hbm.at[part], sem.at[2 * c]),
            pltpu.make_async_copy(rad.at[part], rad_hbm.at[part], sem.at[2 * c + 1]),
        ]
        for copy in group:
            copy.start()
        stores += group
    for copy in stores:
        copy.wait()


def solution(mesh):
    groups, domains = mesh.shape["grp"], mesh.shape["dom"]

    def local(
        positions, velocities, masses, block_halo, block_shift, block_live, block_count, home_slot
    ):
        blocks, width = masses.shape
        halos = home_slot.shape[0]
        owned = halos // (groups * domains)
        near = 3 * domains - 1
        far = (groups - 3) * domains
        vmem = pl.BlockSpec(memory_space=pltpu.VMEM)
        hbm = pl.BlockSpec(memory_space=pl.ANY)
        dma = pltpu.SemaphoreType.DMA
        pos, vel, means, sums = pl.pallas_call(
            functools.partial(exchange_kernel, groups, domains, owned),
            out_shape=(
                pltpu.VMEM((3, blocks, width), F32),
                pltpu.VMEM((3, blocks, width), F32),
                pltpu.VMEM((blocks, LANES), F32),
                pltpu.VMEM((16, owned), F32),
            ),
            in_specs=[hbm] * 8,
            out_specs=(vmem, vmem, vmem, vmem),
            scratch_shapes=[
                pltpu.VMEM((1, blocks), jnp.int32),
                pltpu.VMEM((3, blocks), jnp.int32),
                pltpu.VMEM((1, blocks), jnp.int32),
                pltpu.SMEM((1, 1), jnp.int32),
                pltpu.VMEM((halos // LANES, LANES), jnp.int32),
                pltpu.VMEM((blocks, width), F32),
                pltpu.VMEM((blocks, 1), F32),
                pltpu.VMEM((blocks, LANES), F32),
                pltpu.VMEM((blocks, LANES), F32),
                pltpu.VMEM((16, blocks), F32),
                pltpu.VMEM((1, 1, blocks), F32),
                pltpu.VMEM((near, 16, blocks), F32),
                pltpu.VMEM((far, blocks), F32),
                dma((5,)), dma((3 * CHUNKS,)),
                dma((near,)), dma((near,)),
                dma((far,)), dma((far,)),
            ],
            compiler_params=pltpu.CompilerParams(collective_id=0, has_side_effects=True),
        )(
            positions, velocities, masses,
            block_halo.reshape(1, blocks), block_shift, block_live.reshape(1, blocks),
            block_count.reshape(1, 1), home_slot.reshape(halos // LANES, LANES),
        )
        return pl.pallas_call(
            functools.partial(output_kernel, halos),
            out_shape=(
                jax.ShapeDtypeStruct((11, owned), F32),
                jax.ShapeDtypeStruct((blocks, width), F32),
                jax.ShapeDtypeStruct((blocks, width), F32),
            ),
            in_specs=[vmem, vmem, vmem, vmem],
            out_specs=(hbm, hbm, hbm),
            scratch_shapes=[
                pltpu.VMEM((11, owned), F32),
                pltpu.VMEM((blocks, width), F32),
                pltpu.VMEM((blocks, width), F32),
                dma((2 * CHUNKS + 1,)),
            ],
        )(*[pltpu.with_memory_space_constraint(x, pltpu.VMEM) for x in (pos, vel, means, sums)])

    return jax.shard_map(
        local,
        mesh=mesh,
        in_specs=(
            P(None, ("grp", "dom"), None),
            P(None, ("grp", "dom"), None),
            P(("grp", "dom"), None),
            P(("grp", "dom")),
            P(None, ("grp", "dom")),
            P(("grp", "dom")),
            P(("grp", "dom")),
            P(),
        ),
        out_specs=(P(None, ("grp", "dom")), P(("grp", "dom"), None), P(("grp", "dom"), None)),
        check_vma=False,
    )
```

```python
import functools

import jax
import jax.numpy as jnp
from jax import lax
from jax.experimental import pallas as pl
from jax.experimental.pallas import tpu as pltpu
from jax.sharding import PartitionSpec as P

BOX = 1.0
EPSILON = 1e-06
MESH = pl.DeviceIdType.MESH
F32 = jnp.float32
BF16 = jnp.bfloat16
LANES = 128
CHUNKS = 4
SLOT_ROW = 8
SPIN_ROW = 9
USED_ROWS = 12
SUMS = 11
MASS_ROW = 12


def pieces(x):
    hi = x.astype(BF16).astype(F32)
    rest = x - hi
    mid = rest.astype(BF16).astype(F32)
    return hi, mid, rest - mid


def quotient(x, n):
    return x >> (n.bit_length() - 1) if n & (n - 1) == 0 else x // n


def crossed(a, b):
    return (a[1] * b[2] - a[2] * b[1], a[2] * b[0] - a[0] * b[2], a[0] * b[1] - a[1] * b[0])


def chunk_spans(blocks):
    spans, start = [], 0
    for part in (2, 4, 8, 8):
        rows = max(blocks // part, 8)
        spans.append((start, rows))
        start += rows
    return spans


def exchange_kernel(
    groups, domains, owned,
    pos_hbm, vel_hbm, mass_hbm, halo_hbm, shift_hbm, live_hbm, count_ref, home_hbm,
    pos, vel, means_ref, sums_ref,
    halo_ref, shift_ref, live_ref, home_ref, mass, cols, slots, partial, moments, tile, mass_row, near_in, far_in,
    small_sem, in_sem, send_near, recv_near, send_far, recv_far,
):
    blocks, width = mass.shape
    spans = chunk_spans(blocks)
    g = lax.axis_index("grp")
    d = lax.axis_index("dom")

    def wrapped(x, n):
        return jnp.where(x >= n, x - n, x)

    def peer(dg, dd):
        return {"grp": wrapped(g + dg % groups, groups), "dom": wrapped(d + dd % domains, domains)}

    pairs = (
        (live_hbm, live_ref), (halo_hbm, halo_ref), (home_hbm, home_ref),
        (shift_hbm, shift_ref),
    )
    smalls = [
        pltpu.make_async_copy(src, dst, small_sem.at[k]) for k, (src, dst) in enumerate(pairs)
    ]
    for copy in smalls:
        copy.start()
    ahead = [(1, dd) for dd in range(domains)]
    behind = [(groups - 1, dd) for dd in range(domains)]
    inside = [(0, dd) for dd in range(1, domains)]
    far = [(dg, dd) for dg in range(2, groups - 1) for dd in range(domains)]
    near = ahead + behind + inside
    barrier = pltpu.get_barrier_semaphore()
    peers = near + far
    for dg, dd in peers[:1]:
        pl.semaphore_signal(barrier, inc=1, device_id=peer(dg, dd), device_id_type=MESH)
    loads = []
    for c, (start, rows) in enumerate(spans):
        part = pl.ds(start, rows)
        group = [
            pltpu.make_async_copy(mass_hbm.at[part], mass.at[part], in_sem.at[3 * c]),
            pltpu.make_async_copy(pos_hbm.at[:, part], pos.at[:, part], in_sem.at[3 * c + 1]),
            pltpu.make_async_copy(vel_hbm.at[:, part], vel.at[:, part], in_sem.at[3 * c + 2]),
        ]
        for n, copy in enumerate(group):
            copy.start(priority=1)
        loads.append(group)

    for dg, dd in peers[1:]:
        pl.semaphore_signal(barrier, inc=1, device_id=peer(dg, dd), device_id_type=MESH)

    for copy in smalls:
        copy.wait()

    lane = lax.broadcasted_iota(jnp.int32, (blocks, LANES), 1)
    row = lax.broadcasted_iota(jnp.int32, (blocks, 1), 0)
    packed = jnp.concatenate(
        [
            halo_ref[...].astype(F32),
            live_ref[...].astype(F32),
            jnp.zeros((6, blocks), F32),
        ],
        axis=0,
    )
    turned = packed.T
    live_col = jnp.where(row < count_ref[0], turned[:, 1:2], 0.0)
    cols[...] = jnp.broadcast_to(live_col, (blocks, LANES))

    halo = turned[:, 0:1].astype(jnp.int32)
    home = home_ref[...]
    home_rows = home.shape[0]
    row_pick = lax.broadcasted_iota(jnp.int32, (blocks, home_rows), 1) == quotient(halo, LANES)
    split = jnp.concatenate([(home >> 8).astype(F32), (home & 255).astype(F32)], axis=1)
    picked = jnp.dot(
        row_pick.astype(F32).astype(BF16), split.astype(BF16), preferred_element_type=F32
    )
    value = picked[:, :LANES] * 256.0 + picked[:, LANES:]
    slot = jnp.sum(jnp.where(lane == (halo & (LANES - 1)), value, 0.0), axis=1, keepdims=True)
    slots[...] = jnp.broadcast_to(slot, (blocks, LANES))

    lane8 = lax.broadcasted_iota(jnp.int32, (8, LANES), 1)
    shift = shift_ref[...].astype(F32) * BOX

    def add_up(start):
        at = pl.ds(start, 8)
        live = cols[at]
        sums = None
        for t in range(width // LANES):
            span = pl.ds(t * LANES, LANES)
            place = (lane8 + t * LANES).astype(F32)
            w = jnp.where(place < live, mass[at, span], 0.0)
            x = [pos[k, at, span] for k in range(3)]
            v = [vel[k, at, span] for k in range(3)]
            wv = [w * y for y in v]
            made = [w] + [w * y for y in x] + wv
            made += [wv[0] * v[0] + wv[1] * v[1] + wv[2] * v[2]]
            made += list(crossed(x, wv))
            sums = made if sums is None else [a + b for a, b in zip(sums, made)]
        for k, y in enumerate(sums):
            partial[k, at] = y

    def fold(start):
        at = pl.ds(start, 8)
        out = jnp.where(lane8 == SLOT_ROW, slots[at], 0.0)
        for k in range(SUMS):
            lane_at = k if k < SLOT_ROW else k + 1
            out = jnp.where(lane8 == lane_at, jnp.sum(partial[k, at], axis=1, keepdims=True), out)
        moments[at] = out

    done = []
    for c, (start, rows) in enumerate(spans):
        for copy in loads[c]:
            copy.wait()
        for i in range(start, start + rows, 8):
            add_up(i)
        for i in done:
            fold(i)
        done = range(start, start + rows, 8)
    for i in done:
        fold(i)

    by_row = moments[...].T[:16]
    blank = jnp.zeros((1, blocks), F32)
    s = [shift[k:k + 1] for k in range(3)]
    v = [by_row[4 + k:5 + k] for k in range(3)]

    def stack(x, first):
        return jnp.concatenate([blank] * first + list(x) + [blank] * (5 - first), axis=0)

    first = by_row[0:8] + stack(s, 1) * by_row[0:1]
    turn = stack((s[1], s[2], s[0]), 1) * stack((v[2], v[0], v[1]), 1)
    turn = turn - stack((s[2], s[0], s[1]), 1) * stack((v[1], v[2], v[0]), 1)
    second = by_row[8:16] + turn
    tile[0:8] = first
    tile[8:16] = second
    mass_row[0] = first[0:1]

    pl.semaphore_wait(barrier, len(near) + len(far))

    def near_copy(k, dg, dd):
        part = pl.ds(0, SLOT_ROW + 1) if dg == groups - 1 else pl.ds(0, USED_ROWS)
        return pltpu.make_async_remote_copy(
            src_ref=tile.at[part], dst_ref=near_in.at[k, part],
            send_sem=send_near.at[k], recv_sem=recv_near.at[k],
            device_id=peer(dg, dd), device_id_type=MESH,
        )

    def far_copy(k, dg, dd):
        return pltpu.make_async_remote_copy(
            src_ref=mass_row.at[0], dst_ref=far_in.at[pl.ds(k, 1)],
            send_sem=send_far.at[k], recv_sem=recv_far.at[k],
            device_id=peer(dg, dd), device_id_type=MESH,
        )

    near_copies = [near_copy(k, *p) for k, p in enumerate(near)]
    far_copies = [far_copy(k, *p) for k, p in enumerate(far)]
    from_behind = range(0, domains)
    from_ahead = range(domains, 2 * domains)
    from_inside = range(2 * domains, len(near))
    for copy in near_copies[:2 * domains] + far_copies + near_copies[2 * domains:]:
        copy.start()

    row8 = lax.broadcasted_iota(jnp.int32, (8, blocks), 0)
    base = ((g * domains + d) * owned).astype(F32)
    mine = lax.broadcasted_iota(jnp.int32, (owned, blocks), 0).astype(F32) + base

    def gather(tiles, own):
        left, right = [], []
        for upper, lower in tiles:
            place = lower[0:1]
            hit = (slots[...] == place).astype(F32)
            if own:
                body = jnp.concatenate([upper, jnp.where(row8 < USED_ROWS - 8, lower, 0.0)], axis=0)
                hit = jnp.concatenate([hit, (mine == place).astype(F32)], axis=0)
                left.append(jnp.concatenate(pieces(body), axis=0))
            else:
                left.append(jnp.concatenate(list(pieces(upper)) + [jnp.zeros_like(upper)], axis=0))
            right.append(hit)
        left = jnp.concatenate(left, axis=1).astype(BF16)
        right = jnp.concatenate(right, axis=1).astype(BF16)
        out = lax.dot_general(left, right, (((1,), (1,)), ((), ())), preferred_element_type=F32)
        n = 16 if own else 8
        return out[0:n] + out[n:2 * n] + out[2 * n:3 * n]

    def inbox(ks):
        for k in ks:
            near_copies[k].wait_recv()
        return [(near_in[k, 0:8], near_in[k, 8:16]) for k in ks]

    total = first[0:1]
    tiles = inbox(from_inside)
    total = functools.reduce(lambda a, b: a + b, [t[0][0:1] for t in tiles], total)
    held = gather([(first, second)] + tiles, True)
    means, sums = held[0:8, :blocks], held[:, blocks:]
    tiles = inbox(from_ahead)
    total = functools.reduce(lambda a, b: a + b, [t[0][0:1] for t in tiles], total)
    means = means + gather(tiles, False)
    for copy in near_copies + far_copies:
        copy.wait_send()
    tiles = inbox(from_behind)
    total = functools.reduce(lambda a, b: a + b, [t[0][0:1] for t in tiles], total)
    held = gather(tiles, True)
    means = means + held[0:8, :blocks]
    sums = sums + held[:, blocks:]

    centre, drift, spread = halo_means(means)
    live = jnp.where(
        lax.broadcasted_iota(jnp.int32, (1, blocks), 1) < count_ref[0],
        live_ref[...].astype(F32), 0.0,
    )
    by_block = jnp.concatenate(
        [centre[k] - s[k] for k in range(3)]
        + drift
        + [1.0 / (3.0 * spread + EPSILON), live, jnp.zeros((LANES - 8, blocks), F32)],
        axis=0,
    )
    means_ref[...] = by_block.T

    for copy in far_copies:
        copy.wait_recv()
    if far_copies:
        total = total + jnp.sum(far_in[...], axis=0, keepdims=True)
    sums_ref[0:8] = sums[0:8]
    sums_ref[8:16] = jnp.where(row8 == MASS_ROW - 8, total, sums[8:16])


def halo_means(sums):
    scaled = sums[1:8] * (1.0 / jnp.maximum(sums[0:1], 1.0))
    centre = [scaled[k:k + 1] for k in range(3)]
    drift = [scaled[3 + k:4 + k] for k in range(3)]
    spread = scaled[6:7] - (drift[0] * drift[0] + drift[1] * drift[1] + drift[2] * drift[2])
    return centre, drift, spread


def output_kernel(
    halos, pos, vel, means_ref, sums_ref, table_hbm, kin_hbm, rad_hbm, table, kin, rad, sem
):
    blocks, width = kin.shape
    rows = blocks // CHUNKS
    position8 = lax.broadcasted_iota(jnp.int32, (8, width), 1).astype(F32)

    sums = sums_ref[...]
    centre, drift, spread = halo_means(sums)
    heavy_inv = 1.0 / jnp.maximum(sums[0:1], 1.0)
    turned_spin = crossed(centre, drift)
    spin = [sums[SPIN_ROW + k:SPIN_ROW + 1 + k] * heavy_inv - turned_spin[k] for k in range(3)]
    total = jnp.sum(sums[MASS_ROW:MASS_ROW + 1], axis=1, keepdims=True)
    share = sums[0:1] * float(halos) / total
    table[...] = jnp.concatenate([share] + centre + drift + [spread] + spin, axis=0)
    stores = [pltpu.make_async_copy(table, table_hbm, sem.at[2 * CHUNKS])]
    stores[0].start()

    def output_rows(start):
        at = pl.ds(start, 8)
        mean = means_ref[at]
        live = position8 < mean[:, 7:8]
        kinetic = 0.0
        radial = 0.0
        for k in range(3):
            distance = pos[k, at] - mean[:, k:k + 1]
            radial = radial + distance * distance
            offset = vel[k, at] - mean[:, 3 + k:4 + k]
            kinetic = kinetic + offset * offset
        kin[at] = jnp.where(live, kinetic * mean[:, 6:7], 0.0)
        rad[at] = jnp.where(live, radial, 0.0)

    for c in range(CHUNKS):

        def step(i, carry, c=c):
            output_rows(pl.multiple_of(c * rows + i * 8, 8))
            return carry

        lax.fori_loop(0, rows // 8, step, 0, unroll=True)
        part = pl.ds(c * rows, rows)
        group = [
            pltpu.make_async_copy(kin.at[part], kin_hbm.at[part], sem.at[2 * c]),
            pltpu.make_async_copy(rad.at[part], rad_hbm.at[part], sem.at[2 * c + 1]),
        ]
        for copy in group:
            copy.start()
        stores += group
    for copy in stores:
        copy.wait()


def solution(mesh):
    groups, domains = mesh.shape["grp"], mesh.shape["dom"]

    def local(
        positions, velocities, masses, block_halo, block_shift, block_live, block_count, home_slot
    ):
        blocks, width = masses.shape
        halos = home_slot.shape[0]
        owned = halos // (groups * domains)
        near = 3 * domains - 1
        far = (groups - 3) * domains
        vmem = pl.BlockSpec(memory_space=pltpu.VMEM)
        hbm = pl.BlockSpec(memory_space=pl.ANY)
        dma = pltpu.SemaphoreType.DMA
        pos, vel, means, sums = pl.pallas_call(
            functools.partial(exchange_kernel, groups, domains, owned),
            out_shape=(
                pltpu.VMEM((3, blocks, width), F32),
                pltpu.VMEM((3, blocks, width), F32),
                pltpu.VMEM((blocks, LANES), F32),
                pltpu.VMEM((16, owned), F32),
            ),
            in_specs=[hbm] * 6 + [pl.BlockSpec(memory_space=pltpu.SMEM), hbm],
            out_specs=(vmem, vmem, vmem, vmem),
            scratch_shapes=[
                pltpu.VMEM((1, blocks), jnp.int32),
                pltpu.VMEM((3, blocks), jnp.int32),
                pltpu.VMEM((1, blocks), jnp.int32),
                pltpu.VMEM((halos // LANES, LANES), jnp.int32),
                pltpu.VMEM((blocks, width), F32),
                pltpu.VMEM((blocks, LANES), F32),
                pltpu.VMEM((blocks, LANES), F32),
                pltpu.VMEM((SUMS, blocks, LANES), F32),
                pltpu.VMEM((blocks, LANES), F32),
                pltpu.VMEM((16, blocks), F32),
                pltpu.VMEM((1, 1, blocks), F32),
                pltpu.VMEM((near, 16, blocks), F32),
                pltpu.VMEM((far, blocks), F32),
                dma((4,)), dma((3 * len(chunk_spans(blocks)),)),
                dma((near,)), dma((near,)),
                dma((far,)), dma((far,)),
            ],
            compiler_params=pltpu.CompilerParams(collective_id=0, has_side_effects=True),
        )(
            positions, velocities, masses,
            block_halo.reshape(1, blocks), block_shift, block_live.reshape(1, blocks),
            block_count, home_slot.reshape(halos // LANES, LANES),
        )
        return pl.pallas_call(
            functools.partial(output_kernel, halos),
            out_shape=(
                jax.ShapeDtypeStruct((11, owned), F32),
                jax.ShapeDtypeStruct((blocks, width), F32),
                jax.ShapeDtypeStruct((blocks, width), F32),
            ),
            in_specs=[vmem, vmem, vmem, vmem],
            out_specs=(hbm, hbm, hbm),
            scratch_shapes=[
                pltpu.VMEM((11, owned), F32),
                pltpu.VMEM((blocks, width), F32),
                pltpu.VMEM((blocks, width), F32),
                dma((2 * CHUNKS + 1,)),
            ],
        )(*[pltpu.with_memory_space_constraint(x, pltpu.VMEM) for x in (pos, vel, means, sums)])

    return jax.shard_map(
        local,
        mesh=mesh,
        in_specs=(
            P(None, ("grp", "dom"), None),
            P(None, ("grp", "dom"), None),
            P(("grp", "dom"), None),
            P(("grp", "dom")),
            P(None, ("grp", "dom")),
            P(("grp", "dom")),
            P(("grp", "dom")),
            P(),
        ),
        out_specs=(P(None, ("grp", "dom")), P(("grp", "dom"), None), P(("grp", "dom"), None)),
        check_vma=False,
    )
```

```python
import functools

import jax
import jax.numpy as jnp
from jax import lax
from jax.experimental import pallas as pl
from jax.experimental.pallas import tpu as pltpu
from jax.sharding import PartitionSpec as P

BOX = 1.0
EPSILON = 1e-06
MESH = pl.DeviceIdType.MESH
F32 = jnp.float32
BF16 = jnp.bfloat16
LANES = 128
CHUNKS = 4
SLOT_ROW = 8
SPIN_ROW = 9
USED_ROWS = 12
SUMS = 11
MASS_ROW = 12


def pieces(x):
    hi = x.astype(BF16).astype(F32)
    rest = x - hi
    mid = rest.astype(BF16).astype(F32)
    return hi, mid, rest - mid


def quotient(x, n):
    return x >> (n.bit_length() - 1) if n & (n - 1) == 0 else x // n


def crossed(a, b):
    return (a[1] * b[2] - a[2] * b[1], a[2] * b[0] - a[0] * b[2], a[0] * b[1] - a[1] * b[0])


def chunk_spans(blocks):
    tail = max(blocks // 8, 8)
    middle = max(3 * blocks // 8 // 8 * 8, 8)
    first = blocks - middle - tail
    return [(0, first), (first, middle), (first + middle, tail)]


def exchange_kernel(
    groups, domains, owned,
    pos_hbm, vel_hbm, mass_hbm, halo_hbm, shift_hbm, live_hbm, count_ref, home_hbm,
    pos, vel, means_ref, sums_ref,
    halo_ref, shift_ref, live_ref, home_ref, mass, cols, slots, partial, moments, tile, mass_row, near_in, far_in,
    small_sem, in_sem, send_near, recv_near, send_far, recv_far,
):
    blocks, width = mass.shape
    spans = chunk_spans(blocks)
    g = lax.axis_index("grp")
    d = lax.axis_index("dom")

    def wrapped(x, n):
        return jnp.where(x >= n, x - n, x)

    def peer(dg, dd):
        return {"grp": wrapped(g + dg % groups, groups), "dom": wrapped(d + dd % domains, domains)}

    pairs = (
        (live_hbm, live_ref), (halo_hbm, halo_ref), (home_hbm, home_ref),
        (shift_hbm, shift_ref),
    )
    smalls = [
        pltpu.make_async_copy(src, dst, small_sem) for src, dst in pairs
    ]
    for copy in smalls:
        copy.start()
    turns = sorted(range(domains), key=lambda dd: -min(dd, domains - dd))
    ahead = [(1, dd) for dd in turns]
    behind = [(groups - 1, dd) for dd in turns]
    inside = [(0, dd) for dd in turns[:-1]]
    far = [(dg, dd) for dg in range(2, groups - 1) for dd in turns]
    near = ahead + behind + inside
    barrier = pltpu.get_barrier_semaphore()
    peers = near + far
    for dg, dd in peers[:1]:
        pl.semaphore_signal(barrier, inc=1, device_id=peer(dg, dd), device_id_type=MESH)
    loads = []
    for c, (start, rows) in enumerate(spans):
        part = pl.ds(start, rows)
        group = [
            pltpu.make_async_copy(mass_hbm.at[part], mass.at[part], in_sem.at[c]),
            pltpu.make_async_copy(pos_hbm.at[:, part], pos.at[:, part], in_sem.at[c]),
            pltpu.make_async_copy(vel_hbm.at[:, part], vel.at[:, part], in_sem.at[c]),
        ]
        for copy in group:
            copy.start(priority=1)
        loads.append(group)

    for dg, dd in peers[1:]:
        pl.semaphore_signal(barrier, inc=1, device_id=peer(dg, dd), device_id_type=MESH)

    for copy in smalls:
        copy.wait()

    lane = lax.broadcasted_iota(jnp.int32, (blocks, LANES), 1)
    row = lax.broadcasted_iota(jnp.int32, (blocks, 1), 0)
    packed = jnp.concatenate(
        [
            halo_ref[...].astype(F32),
            live_ref[...].astype(F32),
            jnp.zeros((6, blocks), F32),
        ],
        axis=0,
    )
    turned = packed.T
    live_col = jnp.where(row < count_ref[0], turned[:, 1:2], 0.0)
    cols[...] = jnp.broadcast_to(live_col, (blocks, LANES))

    halo = turned[:, 0:1].astype(jnp.int32)
    home = home_ref[...]
    home_rows = home.shape[0]
    row_pick = lax.broadcasted_iota(jnp.int32, (blocks, home_rows), 1) == quotient(halo, LANES)
    split = jnp.concatenate([(home >> 8).astype(F32), (home & 255).astype(F32)], axis=1)
    picked = jnp.dot(
        row_pick.astype(F32).astype(BF16), split.astype(BF16), preferred_element_type=F32
    )
    value = picked[:, :LANES] * 256.0 + picked[:, LANES:]
    slot = jnp.sum(jnp.where(lane == (halo & (LANES - 1)), value, 0.0), axis=1, keepdims=True)
    slots[...] = jnp.broadcast_to(slot, (blocks, LANES))

    lane8 = lax.broadcasted_iota(jnp.int32, (8, LANES), 1)
    shift = shift_ref[...].astype(F32) * BOX

    def add_up(start):
        at = pl.ds(start, 8)
        live = cols[at]
        sums = None
        for t in range(width // LANES):
            span = pl.ds(t * LANES, LANES)
            place = (lane8 + t * LANES).astype(F32)
            w = jnp.where(place < live, mass[at, span], 0.0)
            x = [pos[k, at, span] for k in range(3)]
            v = [vel[k, at, span] for k in range(3)]
            wv = [w * y for y in v]
            made = [w] + [w * y for y in x] + wv
            made += [wv[0] * v[0] + wv[1] * v[1] + wv[2] * v[2]]
            made += list(crossed(x, wv))
            sums = made if sums is None else [a + b for a, b in zip(sums, made)]
        for k, y in enumerate(sums):
            partial[k, at] = y

    def fold(start):
        at = pl.ds(start, 8)
        out = jnp.where(lane8 == SLOT_ROW, slots[at], 0.0)
        for k in range(SUMS):
            lane_at = k if k < SLOT_ROW else k + 1
            out = jnp.where(lane8 == lane_at, jnp.sum(partial[k, at], axis=1, keepdims=True), out)
        moments[at] = out

    done = []
    for c, (start, rows) in enumerate(spans):
        for copy in loads[c]:
            copy.wait()
        for i in range(start, start + rows, 8):
            add_up(i)
        for i in done:
            fold(i)
        done = range(start, start + rows, 8)
    for i in done:
        fold(i)

    by_row = moments[...].T[:16]
    blank = jnp.zeros((1, blocks), F32)
    s = [shift[k:k + 1] for k in range(3)]
    v = [by_row[4 + k:5 + k] for k in range(3)]

    def stack(x, first):
        return jnp.concatenate([blank] * first + list(x) + [blank] * (5 - first), axis=0)

    first = by_row[0:8] + stack(s, 1) * by_row[0:1]
    turn = stack((s[1], s[2], s[0]), 1) * stack((v[2], v[0], v[1]), 1)
    turn = turn - stack((s[2], s[0], s[1]), 1) * stack((v[1], v[2], v[0]), 1)
    second = by_row[8:16] + turn
    tile[0:8] = first
    tile[8:16] = second
    mass_row[0] = first[0:1]

    pl.semaphore_wait(barrier, len(near) + len(far))

    def remote(src, dst, send, recv, dg, dd):
        return pltpu.make_async_remote_copy(
            src_ref=src, dst_ref=dst, send_sem=send, recv_sem=recv,
            device_id=peer(dg, dd), device_id_type=MESH,
        )

    used = pl.ds(0, USED_ROWS)
    from_behind, from_ahead, from_inside = 0, 1, 2

    def landing(k):
        return near_in.at[pl.ds(k * domains, domains if k < from_inside else domains - 1), used]

    for k, (dg, dd) in enumerate(near[:2 * domains]):
        remote(
            tile.at[used], near_in.at[k, used], send_near, recv_near.at[k // domains], dg, dd
        ).start()
    for k, (dg, dd) in enumerate(far):
        remote(mass_row.at[0], far_in.at[pl.ds(k, 1)], send_far, recv_far, dg, dd).start()
    for k, (dg, dd) in enumerate(near[2 * domains:], 2 * domains):
        remote(
            tile.at[used], near_in.at[k, used], send_near, recv_near.at[k // domains], dg, dd
        ).start()

    row8 = lax.broadcasted_iota(jnp.int32, (8, blocks), 0)
    base = ((g * domains + d) * owned).astype(F32)
    mine = lax.broadcasted_iota(jnp.int32, (owned, blocks), 0).astype(F32) + base

    def gather(tiles, own):
        left, right = [], []
        for upper, lower in tiles:
            place = lower[0:1]
            hit = (slots[...] == place).astype(F32)
            if own:
                body = jnp.concatenate([upper, jnp.where(row8 < USED_ROWS - 8, lower, 0.0)], axis=0)
                hit = jnp.concatenate([hit, (mine == place).astype(F32)], axis=0)
                left.append(jnp.concatenate(pieces(body), axis=0))
            else:
                left.append(jnp.concatenate(list(pieces(upper)) + [jnp.zeros_like(upper)], axis=0))
            right.append(hit)
        left = jnp.concatenate(left, axis=1).astype(BF16)
        right = jnp.concatenate(right, axis=1).astype(BF16)
        out = lax.dot_general(left, right, (((1,), (1,)), ((), ())), preferred_element_type=F32)
        n = 16 if own else 8
        return out[0:n] + out[n:2 * n] + out[2 * n:3 * n]

    def inbox(k):
        whole = landing(k)
        remote(whole, whole, send_near, recv_near.at[k], *near[0]).wait_recv()
        at = range(k * domains, (k + 1) * domains if k < from_inside else len(near))
        return [(near_in[n, 0:8], near_in[n, 8:16]) for n in at]

    def masses_of(tiles):
        return functools.reduce(lambda a, b: a + b, [t[0][0:1] for t in tiles])

    tiles = inbox(from_inside)
    total = first[0:1] + masses_of(tiles)
    held = gather([(first, second)] + tiles, True)
    means, sums = held[0:8, :blocks], held[:, blocks:]
    tiles = inbox(from_ahead)
    total = total + masses_of(tiles)
    means = means + gather(tiles, False)
    whole = near_in.at[:, used]
    remote(whole, whole, send_near, recv_near.at[0], *near[0]).wait_send()
    if far:
        remote(far_in, far_in, send_far, recv_far, *near[0]).wait()
        total = total + jnp.sum(far_in[...], axis=0, keepdims=True)
    tiles = inbox(from_behind)
    total = total + masses_of(tiles)
    held = gather(tiles, True)
    means = means + held[0:8, :blocks]
    sums = sums + held[:, blocks:]

    centre, drift, spread = halo_means(means)
    live = jnp.where(
        lax.broadcasted_iota(jnp.int32, (1, blocks), 1) < count_ref[0],
        live_ref[...].astype(F32), 0.0,
    )
    by_block = jnp.concatenate(
        [centre[k] - s[k] for k in range(3)]
        + drift
        + [1.0 / (3.0 * spread + EPSILON), live],
        axis=0,
    )
    means_ref[:, 0:8] = by_block.T
    sums_ref[0:8] = sums[0:8]
    sums_ref[8:16] = jnp.where(row8 == MASS_ROW - 8, total, sums[8:16])


def halo_means(sums):
    scaled = sums[1:8] * (1.0 / jnp.maximum(sums[0:1], 1.0))
    centre = [scaled[k:k + 1] for k in range(3)]
    drift = [scaled[3 + k:4 + k] for k in range(3)]
    spread = scaled[6:7] - (drift[0] * drift[0] + drift[1] * drift[1] + drift[2] * drift[2])
    return centre, drift, spread


def output_kernel(
    halos, pos, vel, means_ref, sums_ref, table_hbm, kin_hbm, rad_hbm, table, kin, rad, sem
):
    blocks, width = kin.shape
    rows = blocks // CHUNKS
    position8 = lax.broadcasted_iota(jnp.int32, (8, width), 1).astype(F32)

    sums = sums_ref[...]
    centre, drift, spread = halo_means(sums)
    heavy_inv = 1.0 / jnp.maximum(sums[0:1], 1.0)
    turned_spin = crossed(centre, drift)
    spin = [sums[SPIN_ROW + k:SPIN_ROW + 1 + k] * heavy_inv - turned_spin[k] for k in range(3)]
    total = jnp.sum(sums[MASS_ROW:MASS_ROW + 1], axis=1, keepdims=True)
    share = sums[0:1] * float(halos) / total
    table[...] = jnp.concatenate([share] + centre + drift + [spread] + spin, axis=0)
    stores = [pltpu.make_async_copy(table, table_hbm, sem)]
    stores[0].start()

    def output_rows(start):
        at = pl.ds(start, 8)
        mean = means_ref[at]
        live = position8 < mean[:, 7:8]
        kinetic = 0.0
        radial = 0.0
        for k in range(3):
            distance = pos[k, at] - mean[:, k:k + 1]
            radial = radial + distance * distance
            offset = vel[k, at] - mean[:, 3 + k:4 + k]
            kinetic = kinetic + offset * offset
        kin[at] = jnp.where(live, kinetic * mean[:, 6:7], 0.0)
        rad[at] = jnp.where(live, radial, 0.0)

    for c in range(CHUNKS):

        def step(i, carry, c=c):
            output_rows(pl.multiple_of(c * rows + i * 8, 8))
            return carry

        lax.fori_loop(0, rows // 8, step, 0, unroll=True)
        part = pl.ds(c * rows, rows)
        group = [
            pltpu.make_async_copy(kin.at[part], kin_hbm.at[part], sem),
            pltpu.make_async_copy(rad.at[part], rad_hbm.at[part], sem),
        ]
        for copy in group:
            copy.start()
        stores += group
    for copy in stores:
        copy.wait()


def solution(mesh):
    groups, domains = mesh.shape["grp"], mesh.shape["dom"]

    def local(
        positions, velocities, masses, block_halo, block_shift, block_live, block_count, home_slot
    ):
        blocks, width = masses.shape
        halos = home_slot.shape[0]
        owned = halos // (groups * domains)
        near = 3 * domains - 1
        far = (groups - 3) * domains
        vmem = pl.BlockSpec(memory_space=pltpu.VMEM)
        hbm = pl.BlockSpec(memory_space=pl.ANY)
        dma = pltpu.SemaphoreType.DMA
        pos, vel, means, sums = pl.pallas_call(
            functools.partial(exchange_kernel, groups, domains, owned),
            out_shape=(
                pltpu.VMEM((3, blocks, width), F32),
                pltpu.VMEM((3, blocks, width), F32),
                pltpu.VMEM((blocks, LANES), F32),
                pltpu.VMEM((16, owned), F32),
            ),
            in_specs=[hbm] * 6 + [pl.BlockSpec(memory_space=pltpu.SMEM), hbm],
            out_specs=(vmem, vmem, vmem, vmem),
            scratch_shapes=[
                pltpu.VMEM((1, blocks), jnp.int32),
                pltpu.VMEM((3, blocks), jnp.int32),
                pltpu.VMEM((1, blocks), jnp.int32),
                pltpu.VMEM((halos // LANES, LANES), jnp.int32),
                pltpu.VMEM((blocks, width), F32),
                pltpu.VMEM((blocks, LANES), F32),
                pltpu.VMEM((blocks, LANES), F32),
                pltpu.VMEM((SUMS, blocks, LANES), F32),
                pltpu.VMEM((blocks, LANES), F32),
                pltpu.VMEM((16, blocks), F32),
                pltpu.VMEM((1, 1, blocks), F32),
                pltpu.VMEM((near, 16, blocks), F32),
                pltpu.VMEM((far, blocks), F32),
                dma, dma((len(chunk_spans(blocks)),)),
                dma, dma((3,)),
                dma, dma,
            ],
            compiler_params=pltpu.CompilerParams(collective_id=0, has_side_effects=True),
        )(
            positions, velocities, masses,
            block_halo.reshape(1, blocks), block_shift, block_live.reshape(1, blocks),
            block_count, home_slot.reshape(halos // LANES, LANES),
        )
        return pl.pallas_call(
            functools.partial(output_kernel, halos),
            out_shape=(
                jax.ShapeDtypeStruct((11, owned), F32),
                jax.ShapeDtypeStruct((blocks, width), F32),
                jax.ShapeDtypeStruct((blocks, width), F32),
            ),
            in_specs=[vmem, vmem, vmem, vmem],
            out_specs=(hbm, hbm, hbm),
            scratch_shapes=[
                pltpu.VMEM((11, owned), F32),
                pltpu.VMEM((blocks, width), F32),
                pltpu.VMEM((blocks, width), F32),
                dma,
            ],
        )(*[pltpu.with_memory_space_constraint(x, pltpu.VMEM) for x in (pos, vel, means, sums)])

    return jax.shard_map(
        local,
        mesh=mesh,
        in_specs=(
            P(None, ("grp", "dom"), None),
            P(None, ("grp", "dom"), None),
            P(("grp", "dom"), None),
            P(("grp", "dom")),
            P(None, ("grp", "dom")),
            P(("grp", "dom")),
            P(("grp", "dom")),
            P(),
        ),
        out_specs=(P(None, ("grp", "dom")), P(("grp", "dom"), None), P(("grp", "dom"), None)),
        check_vma=False,
    )
```

```python
import functools

import jax
import jax.numpy as jnp
from jax import lax
from jax.experimental import pallas as pl
from jax.experimental.pallas import tpu as pltpu
from jax.sharding import PartitionSpec as P

BOX = 1.0
EPSILON = 1e-06
MESH = pl.DeviceIdType.MESH
F32 = jnp.float32
BF16 = jnp.bfloat16
LANES = 128
CHUNKS = 4
SLOT_ROW = 8
SPIN_ROW = 9
USED_ROWS = 12
SUMS = 11
MASS_ROW = 12


def pieces(x):
    hi = x.astype(BF16).astype(F32)
    rest = x - hi
    mid = rest.astype(BF16).astype(F32)
    return hi, mid, rest - mid


def quotient(x, n):
    return x >> (n.bit_length() - 1) if n & (n - 1) == 0 else x // n


def crossed(a, b):
    return (a[1] * b[2] - a[2] * b[1], a[2] * b[0] - a[0] * b[2], a[0] * b[1] - a[1] * b[0])


def chunk_spans(blocks):
    tail = max(blocks // 8, 8)
    middle = max(3 * blocks // 8 // 8 * 8, 8)
    first = blocks - middle - tail
    return [(0, first), (first, middle), (first + middle, tail)]


def exchange_kernel(
    groups, domains, owned,
    pos_hbm, vel_hbm, mass_hbm, halo_hbm, shift_hbm, live_hbm, count_ref, home_hbm,
    pos, vel, means_ref, sums_ref, cols,
    halo_ref, shift_ref, live_ref, home_ref, mass, slots, partial, moments, tile, mass_row, near_in, far_in,
    small_sem, in_sem, recv_sem,
):
    blocks, width = mass.shape
    spans = chunk_spans(blocks)
    g = lax.axis_index("grp")
    d = lax.axis_index("dom")

    def wrapped(x, n):
        return jnp.where(x >= n, x - n, x)

    def peer(dg, dd):
        return {"grp": wrapped(g + dg % groups, groups), "dom": wrapped(d + dd % domains, domains)}

    pairs = (
        (live_hbm, live_ref), (halo_hbm, halo_ref), (home_hbm, home_ref),
        (shift_hbm, shift_ref),
    )
    smalls = [
        pltpu.make_async_copy(src, dst, small_sem) for src, dst in pairs
    ]
    for copy in smalls:
        copy.start()
    turns = sorted(range(domains), key=lambda dd: -min(dd, domains - dd))
    ahead = [(1, dd) for dd in turns]
    behind = [(groups - 1, dd) for dd in turns]
    inside = [(0, dd) for dd in turns[:-1]]
    far = [(dg, dd) for dg in range(2, groups - 1) for dd in turns]
    near = ahead + behind + inside
    barrier = pltpu.get_barrier_semaphore()
    peers = near + far
    for dg, dd in peers[:1]:
        pl.semaphore_signal(barrier, inc=1, device_id=peer(dg, dd), device_id_type=MESH)
    loads = []
    for c, (start, rows) in enumerate(spans):
        part = pl.ds(start, rows)
        group = [
            pltpu.make_async_copy(mass_hbm.at[part], mass.at[part], in_sem.at[c]),
            pltpu.make_async_copy(pos_hbm.at[:, part], pos.at[:, part], in_sem.at[c]),
            pltpu.make_async_copy(vel_hbm.at[:, part], vel.at[:, part], in_sem.at[c]),
        ]
        for copy in group:
            copy.start(priority=1)
        loads.append(group)

    for dg, dd in peers[1:]:
        pl.semaphore_signal(barrier, inc=1, device_id=peer(dg, dd), device_id_type=MESH)

    for copy in smalls:
        copy.wait()

    lane = lax.broadcasted_iota(jnp.int32, (blocks, LANES), 1)
    row = lax.broadcasted_iota(jnp.int32, (blocks, 1), 0)
    packed = jnp.concatenate(
        [
            halo_ref[...].astype(F32),
            live_ref[...].astype(F32),
            jnp.zeros((6, blocks), F32),
        ],
        axis=0,
    )
    turned = packed.T
    live_col = jnp.where(row < count_ref[0], turned[:, 1:2], 0.0)
    cols[...] = jnp.broadcast_to(live_col, (blocks, LANES))

    halo = turned[:, 0:1].astype(jnp.int32)
    home = home_ref[...]
    home_rows = home.shape[0]
    row_pick = lax.broadcasted_iota(jnp.int32, (blocks, home_rows), 1) == quotient(halo, LANES)
    split = jnp.concatenate([(home >> 8).astype(F32), (home & 255).astype(F32)], axis=1)
    picked = jnp.dot(
        row_pick.astype(F32).astype(BF16), split.astype(BF16), preferred_element_type=F32
    )
    value = picked[:, :LANES] * 256.0 + picked[:, LANES:]
    slot = jnp.sum(jnp.where(lane == (halo & (LANES - 1)), value, 0.0), axis=1, keepdims=True)
    slots[...] = jnp.broadcast_to(slot, (blocks, LANES))

    lane8 = lax.broadcasted_iota(jnp.int32, (8, LANES), 1)
    shift = shift_ref[...].astype(F32) * BOX

    def add_up(start):
        at = pl.ds(start, 8)
        live = cols[at]
        sums = None
        for t in range(width // LANES):
            span = pl.ds(t * LANES, LANES)
            place = (lane8 + t * LANES).astype(F32)
            w = jnp.where(place < live, mass[at, span], 0.0)
            x = [pos[k, at, span] for k in range(3)]
            v = [vel[k, at, span] for k in range(3)]
            wv = [w * y for y in v]
            made = [w] + [w * y for y in x] + wv
            made += [wv[0] * v[0] + wv[1] * v[1] + wv[2] * v[2]]
            made += list(crossed(x, wv))
            sums = made if sums is None else [a + b for a, b in zip(sums, made)]
        for k, y in enumerate(sums):
            partial[k, at] = y

    def fold(start):
        at = pl.ds(start, 8)
        out = jnp.where(lane8 == SLOT_ROW, slots[at], 0.0)
        for k in range(SUMS):
            lane_at = k if k < SLOT_ROW else k + 1
            out = jnp.where(lane8 == lane_at, jnp.sum(partial[k, at], axis=1, keepdims=True), out)
        moments[at] = out

    for c, (start, rows) in enumerate(spans):
        for copy in loads[c]:
            copy.wait()
        for i in range(start, start + rows, 8):
            add_up(i)
            fold(i)

    by_row = moments[...].T[:16]
    blank = jnp.zeros((1, blocks), F32)
    s = [shift[k:k + 1] for k in range(3)]
    v = [by_row[4 + k:5 + k] for k in range(3)]

    def stack(x, first):
        return jnp.concatenate([blank] * first + list(x) + [blank] * (5 - first), axis=0)

    first = by_row[0:8] + stack(s, 1) * by_row[0:1]
    turn = stack((s[1], s[2], s[0]), 1) * stack((v[2], v[0], v[1]), 1)
    turn = turn - stack((s[2], s[0], s[1]), 1) * stack((v[1], v[2], v[0]), 1)
    second = by_row[8:16] + turn
    tile[0:8] = first
    tile[8:16] = second
    mass_row[0] = first[0:1]

    pl.semaphore_wait(barrier, len(near) + len(far))

    def remote(src, dst, send, recv, dg, dd):
        return pltpu.make_async_remote_copy(
            src_ref=src, dst_ref=dst, send_sem=send, recv_sem=recv,
            device_id=peer(dg, dd), device_id_type=MESH,
        )

    used = pl.ds(0, USED_ROWS)
    from_behind, from_ahead, from_inside = 0, 1, 2
    send, send_far = in_sem.at[0], in_sem.at[1]
    late, early, recv_far = (recv_sem.at[k] for k in range(3))

    def send_near(first, last):
        for k in range(first, last):
            recv = late if k < domains else early
            remote(tile.at[used], near_in.at[k, used], send, recv, *near[k]).start()

    send_near(0, 2 * domains)
    for k, (dg, dd) in enumerate(far):
        remote(mass_row.at[0], far_in.at[pl.ds(k, 1)], send_far, recv_far, dg, dd).start()
    send_near(2 * domains, len(near))

    row8 = lax.broadcasted_iota(jnp.int32, (8, blocks), 0)
    base = ((g * domains + d) * owned).astype(F32)
    mine = lax.broadcasted_iota(jnp.int32, (owned, blocks), 0).astype(F32) + base

    def gather(tiles, own):
        left, right = [], []
        for upper, lower in tiles:
            place = lower[0:1]
            hit = (slots[...] == place).astype(F32)
            if own:
                body = jnp.concatenate([upper, jnp.where(row8 < USED_ROWS - 8, lower, 0.0)], axis=0)
                hit = jnp.concatenate([hit, (mine == place).astype(F32)], axis=0)
                left.append(jnp.concatenate(pieces(body), axis=0))
            else:
                left.append(jnp.concatenate(list(pieces(upper)) + [jnp.zeros_like(upper)], axis=0))
            right.append(hit)
        left = jnp.concatenate(left, axis=1).astype(BF16)
        right = jnp.concatenate(right, axis=1).astype(BF16)
        out = lax.dot_general(left, right, (((1,), (1,)), ((), ())), preferred_element_type=F32)
        n = 16 if own else 8
        return out[0:n] + out[n:2 * n] + out[2 * n:3 * n]

    def landed(ref, recv):
        remote(ref, ref, send, recv, *near[0]).wait_recv()

    def inbox(k):
        at = range(k * domains, (k + 1) * domains if k < from_inside else len(near))
        return [(near_in[n, 0:8], near_in[n, 8:16]) for n in at]

    def masses_of(tiles):
        return functools.reduce(lambda a, b: a + b, [t[0][0:1] for t in tiles])

    landed(near_in.at[pl.ds(domains, len(near) - domains), used], early)
    if far:
        landed(far_in, recv_far)
    tiles = inbox(from_inside)
    total = first[0:1] + masses_of(tiles)
    held = gather([(first, second)] + tiles, True)
    means, sums = held[0:8, :blocks], held[:, blocks:]
    tiles = inbox(from_ahead)
    total = total + masses_of(tiles)
    means = means + gather(tiles, False)
    whole = near_in.at[:, used]
    remote(whole, whole, send, early, *near[0]).wait_send()
    if far:
        remote(far_in, far_in, send_far, recv_far, *near[0]).wait_send()
        total = total + jnp.sum(far_in[...], axis=0, keepdims=True)
    landed(near_in.at[pl.ds(0, domains), used], late)
    tiles = inbox(from_behind)
    total = total + masses_of(tiles)
    held = gather(tiles, True)
    means = means + held[0:8, :blocks]
    sums = sums + held[:, blocks:]

    centre, drift, spread = halo_means(means)
    by_block = jnp.concatenate(
        [centre[k] - s[k] for k in range(3)]
        + drift
        + [1.0 / (3.0 * spread + EPSILON), blank],
        axis=0,
    )
    means_ref[:, 0:8] = by_block.T
    sums_ref[0:8] = sums[0:8]
    sums_ref[8:16] = jnp.where(row8 == MASS_ROW - 8, total, sums[8:16])


def halo_means(sums):
    scaled = sums[1:8] * (1.0 / jnp.maximum(sums[0:1], 1.0))
    centre = [scaled[k:k + 1] for k in range(3)]
    drift = [scaled[3 + k:4 + k] for k in range(3)]
    spread = scaled[6:7] - (drift[0] * drift[0] + drift[1] * drift[1] + drift[2] * drift[2])
    return centre, drift, spread


def output_kernel(
    halos, pos, vel, means_ref, sums_ref, live_ref, table_hbm, kin_hbm, rad_hbm, table, kin, rad, sem
):
    blocks, width = kin.shape
    rows = blocks // CHUNKS
    stores = []

    lane8 = lax.broadcasted_iota(jnp.int32, (8, LANES), 1)

    def output_rows(start):
        at = pl.ds(start, 8)
        mean = means_ref[at]
        mean = [jnp.broadcast_to(mean[:, k:k + 1], (8, LANES)) for k in range(7)]
        live = live_ref[at]
        for t in range(width // LANES):
            span = pl.ds(t * LANES, LANES)
            kinetic, radial = 0.0, 0.0
            for k in range(3):
                distance = pos[k, at, span] - mean[k]
                radial = radial + distance * distance
                offset = vel[k, at, span] - mean[3 + k]
                kinetic = kinetic + offset * offset
            kept = (lane8 + t * LANES).astype(F32) < live
            kin[at, span] = jnp.where(kept, kinetic * mean[6], 0.0)
            rad[at, span] = jnp.where(kept, radial, 0.0)

    def make_table():
        sums = sums_ref[...]
        centre, drift, spread = halo_means(sums)
        heavy_inv = 1.0 / jnp.maximum(sums[0:1], 1.0)
        turned_spin = crossed(centre, drift)
        spin = [sums[SPIN_ROW + k:SPIN_ROW + 1 + k] * heavy_inv - turned_spin[k] for k in range(3)]
        total = jnp.sum(sums[MASS_ROW:MASS_ROW + 1], axis=1, keepdims=True)
        share = sums[0:1] * float(halos) / total
        table[...] = jnp.concatenate([share] + centre + drift + [spread] + spin, axis=0)
        copy = pltpu.make_async_copy(table, table_hbm, sem)
        copy.start()
        return copy

    for c in range(CHUNKS):

        def step(i, carry, c=c):
            output_rows(pl.multiple_of(c * rows + i * 8, 8))
            return carry

        lax.fori_loop(0, rows // 8, step, 0, unroll=True)
        part = pl.ds(c * rows, rows)
        group = [
            pltpu.make_async_copy(kin.at[part], kin_hbm.at[part], sem),
            pltpu.make_async_copy(rad.at[part], rad_hbm.at[part], sem),
        ]
        for copy in group:
            copy.start()
        stores += group
        if c == 1:
            stores.append(make_table())
    for copy in stores:
        copy.wait()


def solution(mesh):
    groups, domains = mesh.shape["grp"], mesh.shape["dom"]

    def local(
        positions, velocities, masses, block_halo, block_shift, block_live, block_count, home_slot
    ):
        blocks, width = masses.shape
        halos = home_slot.shape[0]
        owned = halos // (groups * domains)
        near = 3 * domains - 1
        far = (groups - 3) * domains
        vmem = pl.BlockSpec(memory_space=pltpu.VMEM)
        hbm = pl.BlockSpec(memory_space=pl.ANY)
        dma = pltpu.SemaphoreType.DMA
        pos, vel, means, sums, live = pl.pallas_call(
            functools.partial(exchange_kernel, groups, domains, owned),
            out_shape=(
                pltpu.VMEM((3, blocks, width), F32),
                pltpu.VMEM((3, blocks, width), F32),
                pltpu.VMEM((blocks, LANES), F32),
                pltpu.VMEM((16, owned), F32),
                pltpu.VMEM((blocks, LANES), F32),
            ),
            in_specs=[hbm] * 6 + [pl.BlockSpec(memory_space=pltpu.SMEM), hbm],
            out_specs=(vmem,) * 5,
            scratch_shapes=[
                pltpu.VMEM((1, blocks), jnp.int32),
                pltpu.VMEM((3, blocks), jnp.int32),
                pltpu.VMEM((1, blocks), jnp.int32),
                pltpu.VMEM((halos // LANES, LANES), jnp.int32),
                pltpu.VMEM((blocks, width), F32),
                pltpu.VMEM((blocks, LANES), F32),
                pltpu.VMEM((SUMS, blocks, LANES), F32),
                pltpu.VMEM((blocks, LANES), F32),
                pltpu.VMEM((16, blocks), F32),
                pltpu.VMEM((1, 1, blocks), F32),
                pltpu.VMEM((near, 16, blocks), F32),
                pltpu.VMEM((far, blocks), F32),
                dma, dma((len(chunk_spans(blocks)),)),
                dma((3,)),
            ],
            compiler_params=pltpu.CompilerParams(collective_id=0, has_side_effects=True),
        )(
            positions, velocities, masses,
            block_halo.reshape(1, blocks), block_shift, block_live.reshape(1, blocks),
            block_count, home_slot.reshape(halos // LANES, LANES),
        )
        return pl.pallas_call(
            functools.partial(output_kernel, halos),
            out_shape=(
                jax.ShapeDtypeStruct((11, owned), F32),
                jax.ShapeDtypeStruct((blocks, width), F32),
                jax.ShapeDtypeStruct((blocks, width), F32),
            ),
            in_specs=[vmem] * 5,
            out_specs=(hbm, hbm, hbm),
            scratch_shapes=[
                pltpu.VMEM((11, owned), F32),
                pltpu.VMEM((blocks, width), F32),
                pltpu.VMEM((blocks, width), F32),
                dma,
            ],
        )(*[pltpu.with_memory_space_constraint(x, pltpu.VMEM) for x in (pos, vel, means, sums, live)])

    return jax.shard_map(
        local,
        mesh=mesh,
        in_specs=(
            P(None, ("grp", "dom"), None),
            P(None, ("grp", "dom"), None),
            P(("grp", "dom"), None),
            P(("grp", "dom")),
            P(None, ("grp", "dom")),
            P(("grp", "dom")),
            P(("grp", "dom")),
            P(),
        ),
        out_specs=(P(None, ("grp", "dom")), P(("grp", "dom"), None), P(("grp", "dom"), None)),
        check_vma=False,
    )
```

```python
import functools

import jax
import jax.numpy as jnp
from jax import lax
from jax.experimental import pallas as pl
from jax.experimental.pallas import tpu as pltpu
from jax.sharding import PartitionSpec as P

BOX = 1.0
EPSILON = 1e-06
MESH = pl.DeviceIdType.MESH
F32 = jnp.float32
BF16 = jnp.bfloat16
LANES = 128
CHUNKS = 4
SLOT_ROW = 8
SPIN_ROW = 9
USED_ROWS = 12
SUMS = 11
MASS_ROW = 12


def pieces(x):
    hi = x.astype(BF16).astype(F32)
    rest = x - hi
    mid = rest.astype(BF16).astype(F32)
    return hi, mid, rest - mid


def quotient(x, n):
    return x >> (n.bit_length() - 1) if n & (n - 1) == 0 else x // n


def crossed(a, b):
    return (a[1] * b[2] - a[2] * b[1], a[2] * b[0] - a[0] * b[2], a[0] * b[1] - a[1] * b[0])


def chunk_spans(blocks):
    tail = max(blocks // 8, 8)
    middle = max(3 * blocks // 8 // 8 * 8, 8)
    first = blocks - middle - tail
    return [(0, first), (first, middle), (first + middle, tail)]


def exchange_kernel(
    groups, domains, owned,
    pos_hbm, vel_hbm, mass_hbm, halo_hbm, shift_hbm, live_hbm, count_ref, home_hbm,
    pos, vel, means_ref, sums_ref, cols,
    halo_ref, shift_ref, live_ref, home_ref, mass, slots, partial, moments, tile, mass_row, near_in, far_in,
    recv_sem, small_sem=None, in_sem=None,
):
    blocks, width = mass.shape
    spans = chunk_spans(blocks)
    g = lax.axis_index("grp")
    d = lax.axis_index("dom")

    def wrapped(x, n):
        return jnp.where(x >= n, x - n, x)

    def peer(dg, dd):
        return {"grp": wrapped(g + dg % groups, groups), "dom": wrapped(d + dd % domains, domains)}

    pairs = (
        (live_hbm, live_ref), (halo_hbm, halo_ref), (home_hbm, home_ref),
        (shift_hbm, shift_ref),
    )
    smalls = [
        pltpu.make_async_copy(src, dst, small_sem) for src, dst in pairs
    ]
    for copy in smalls:
        copy.start()
    turns = sorted(range(domains), key=lambda dd: -min(dd, domains - dd))
    ahead = [(1, dd) for dd in turns]
    behind = [(groups - 1, dd) for dd in turns]
    inside = [(0, dd) for dd in turns[:-1]]
    far = [(dg, dd) for dg in range(2, groups - 1) for dd in turns]
    near = ahead + behind + inside
    barrier = pltpu.get_barrier_semaphore()
    peers = near + far
    for dg, dd in peers[:1]:
        pl.semaphore_signal(barrier, inc=1, device_id=peer(dg, dd), device_id_type=MESH)
    loads = []
    for c, (start, rows) in enumerate(spans):
        part = pl.ds(start, rows)
        group = [
            pltpu.make_async_copy(mass_hbm.at[part], mass.at[part], in_sem.at[c]),
            pltpu.make_async_copy(pos_hbm.at[:, part], pos.at[:, part], in_sem.at[c]),
            pltpu.make_async_copy(vel_hbm.at[:, part], vel.at[:, part], in_sem.at[c]),
        ]
        for copy in group:
            copy.start(priority=1)
        loads.append(group)

    for dg, dd in peers[1:]:
        pl.semaphore_signal(barrier, inc=1, device_id=peer(dg, dd), device_id_type=MESH)

    for copy in smalls:
        copy.wait()

    lane = lax.broadcasted_iota(jnp.int32, (blocks, LANES), 1)
    row = lax.broadcasted_iota(jnp.int32, (blocks, 1), 0)
    packed = jnp.concatenate(
        [
            halo_ref[...].astype(F32),
            live_ref[...].astype(F32),
            jnp.zeros((6, blocks), F32),
        ],
        axis=0,
    )
    turned = packed.T
    live_col = jnp.where(row < count_ref[0], turned[:, 1:2], 0.0)
    cols[...] = jnp.broadcast_to(live_col, (blocks, LANES))

    halo = turned[:, 0:1].astype(jnp.int32)
    home = home_ref[...]
    home_rows = home.shape[0]
    row_pick = lax.broadcasted_iota(jnp.int32, (blocks, home_rows), 1) == quotient(halo, LANES)
    split = jnp.concatenate([(home >> 8).astype(F32), (home & 255).astype(F32)], axis=1)
    picked = jnp.dot(
        row_pick.astype(F32).astype(BF16), split.astype(BF16), preferred_element_type=F32
    )
    value = picked[:, :LANES] * 256.0 + picked[:, LANES:]
    slot = jnp.sum(jnp.where(lane == (halo & (LANES - 1)), value, 0.0), axis=1, keepdims=True)
    slots[...] = jnp.broadcast_to(slot, (blocks, LANES))

    lane8 = lax.broadcasted_iota(jnp.int32, (8, LANES), 1)
    shift = shift_ref[...].astype(F32) * BOX

    def add_up(start):
        at = pl.ds(start, 8)
        live = cols[at]
        sums = None
        for t in range(width // LANES):
            span = pl.ds(t * LANES, LANES)
            place = (lane8 + t * LANES).astype(F32)
            w = jnp.where(place < live, mass[at, span], 0.0)
            x = [pos[k, at, span] for k in range(3)]
            v = [vel[k, at, span] for k in range(3)]
            wv = [w * y for y in v]
            made = [w] + [w * y for y in x] + wv
            made += [wv[0] * v[0] + wv[1] * v[1] + wv[2] * v[2]]
            made += list(crossed(x, wv))
            sums = made if sums is None else [a + b for a, b in zip(sums, made)]
        for k, y in enumerate(sums):
            partial[k, at] = y

    def fold(start):
        at = pl.ds(start, 8)
        out = jnp.where(lane8 == SLOT_ROW, slots[at], 0.0)
        for k in range(SUMS):
            lane_at = k if k < SLOT_ROW else k + 1
            out = jnp.where(lane8 == lane_at, jnp.sum(partial[k, at], axis=1, keepdims=True), out)
        moments[at] = out

    for c, (start, rows) in enumerate(spans):
        for copy in loads[c]:
            copy.wait()
        for i in range(start, start + rows, 8):
            add_up(i)
            fold(i)

    by_row = moments[...].T[:16]
    blank = jnp.zeros((1, blocks), F32)
    s = [shift[k:k + 1] for k in range(3)]
    v = [by_row[4 + k:5 + k] for k in range(3)]

    def stack(x, first):
        return jnp.concatenate([blank] * first + list(x) + [blank] * (5 - first), axis=0)

    first = by_row[0:8] + stack(s, 1) * by_row[0:1]
    turn = stack((s[1], s[2], s[0]), 1) * stack((v[2], v[0], v[1]), 1)
    turn = turn - stack((s[2], s[0], s[1]), 1) * stack((v[1], v[2], v[0]), 1)
    second = by_row[8:16] + turn
    tile[0:8] = first
    tile[8:16] = second
    mass_row[0] = first[0:1]

    pl.semaphore_wait(barrier, len(near) + len(far))

    def remote(src, dst, send, recv, dg, dd):
        return pltpu.make_async_remote_copy(
            src_ref=src, dst_ref=dst, send_sem=send, recv_sem=recv,
            device_id=peer(dg, dd), device_id_type=MESH,
        )

    used = pl.ds(0, USED_ROWS)
    from_behind, from_ahead, from_inside = 0, 1, 2
    send, send_far = in_sem.at[0], in_sem.at[1]
    late, early, recv_far = (recv_sem.at[k] for k in range(3))

    def send_near(first, last):
        for k in range(first, last):
            recv = late if k < domains else early
            remote(tile.at[used], near_in.at[k, used], send, recv, *near[k]).start()

    send_near(0, 2 * domains)
    for k, (dg, dd) in enumerate(far):
        remote(mass_row.at[0], far_in.at[pl.ds(k, 1)], send_far, recv_far, dg, dd).start()
    send_near(2 * domains, len(near))

    row8 = lax.broadcasted_iota(jnp.int32, (8, blocks), 0)
    base = ((g * domains + d) * owned).astype(F32)
    mine = lax.broadcasted_iota(jnp.int32, (owned, blocks), 0).astype(F32) + base

    def gather(tiles, own):
        left, right = [], []
        for upper, lower in tiles:
            place = lower[0:1]
            hit = (slots[...] == place).astype(F32)
            if own:
                body = jnp.concatenate([upper, jnp.where(row8 < USED_ROWS - 8, lower, 0.0)], axis=0)
                hit = jnp.concatenate([hit, (mine == place).astype(F32)], axis=0)
                left.append(jnp.concatenate(pieces(body), axis=0))
            else:
                left.append(jnp.concatenate(list(pieces(upper)) + [jnp.zeros_like(upper)], axis=0))
            right.append(hit)
        left = jnp.concatenate(left, axis=1).astype(BF16)
        right = jnp.concatenate(right, axis=1).astype(BF16)
        out = lax.dot_general(left, right, (((1,), (1,)), ((), ())), preferred_element_type=F32)
        n = 16 if own else 8
        return out[0:n] + out[n:2 * n] + out[2 * n:3 * n]

    def landed(ref, recv):
        remote(ref, ref, send, recv, *near[0]).wait_recv()

    def inbox(k):
        at = range(k * domains, (k + 1) * domains if k < from_inside else len(near))
        return [(near_in[n, 0:8], near_in[n, 8:16]) for n in at]

    def masses_of(tiles):
        return functools.reduce(lambda a, b: a + b, [t[0][0:1] for t in tiles])

    landed(near_in.at[pl.ds(domains, len(near) - domains), used], early)
    if far:
        landed(far_in, recv_far)
    tiles = inbox(from_inside)
    total = first[0:1] + masses_of(tiles)
    held = gather([(first, second)] + tiles, True)
    means, sums = held[0:8, :blocks], held[:, blocks:]
    tiles = inbox(from_ahead)
    total = total + masses_of(tiles)
    means = means + gather(tiles, False)
    whole = near_in.at[:, used]
    remote(whole, whole, send, early, *near[0]).wait_send()
    if far:
        remote(far_in, far_in, send_far, recv_far, *near[0]).wait_send()
        total = total + jnp.sum(far_in[...], axis=0, keepdims=True)
    landed(near_in.at[pl.ds(0, domains), used], late)
    tiles = inbox(from_behind)
    total = total + masses_of(tiles)
    held = gather(tiles, True)
    means = means + held[0:8, :blocks]
    sums = sums + held[:, blocks:]

    centre, drift, spread = halo_means(means)
    by_block = jnp.concatenate(
        [centre[k] - s[k] for k in range(3)]
        + drift
        + [1.0 / (3.0 * spread + EPSILON), blank],
        axis=0,
    )
    means_ref[:, 0:8] = by_block.T
    sums_ref[0:8] = sums[0:8]
    sums_ref[8:16] = jnp.where(row8 == MASS_ROW - 8, total, sums[8:16])


def scoped_exchange(groups, domains, owned, chunks, *refs):
    dma = pltpu.SemaphoreType.DMA
    pl.run_scoped(
        lambda small_sem, in_sem: exchange_kernel(
            groups, domains, owned, *refs, small_sem=small_sem, in_sem=in_sem
        ),
        dma, dma((chunks,)),
    )


def halo_means(sums):
    scaled = sums[1:8] * (1.0 / jnp.maximum(sums[0:1], 1.0))
    centre = [scaled[k:k + 1] for k in range(3)]
    drift = [scaled[3 + k:4 + k] for k in range(3)]
    spread = scaled[6:7] - (drift[0] * drift[0] + drift[1] * drift[1] + drift[2] * drift[2])
    return centre, drift, spread


def output_kernel(
    halos, pos, vel, means_ref, sums_ref, live_ref, table_hbm, kin_hbm, rad_hbm, table, kin, rad, sem=None
):
    blocks, width = kin.shape
    rows = blocks // CHUNKS
    stores = []

    lane8 = lax.broadcasted_iota(jnp.int32, (8, LANES), 1)

    def output_rows(start):
        at = pl.ds(start, 8)
        mean = means_ref[at]
        mean = [jnp.broadcast_to(mean[:, k:k + 1], (8, LANES)) for k in range(7)]
        live = live_ref[at]
        for t in range(width // LANES):
            span = pl.ds(t * LANES, LANES)
            kinetic, radial = 0.0, 0.0
            for k in range(3):
                distance = pos[k, at, span] - mean[k]
                radial = radial + distance * distance
                offset = vel[k, at, span] - mean[3 + k]
                kinetic = kinetic + offset * offset
            kept = (lane8 + t * LANES).astype(F32) < live
            kin[at, span] = jnp.where(kept, kinetic * mean[6], 0.0)
            rad[at, span] = jnp.where(kept, radial, 0.0)

    def make_table():
        sums = sums_ref[...]
        centre, drift, spread = halo_means(sums)
        heavy_inv = 1.0 / jnp.maximum(sums[0:1], 1.0)
        turned_spin = crossed(centre, drift)
        spin = [sums[SPIN_ROW + k:SPIN_ROW + 1 + k] * heavy_inv - turned_spin[k] for k in range(3)]
        total = jnp.sum(sums[MASS_ROW:MASS_ROW + 1], axis=1, keepdims=True)
        share = sums[0:1] * float(halos) / total
        table[...] = jnp.concatenate([share] + centre + drift + [spread] + spin, axis=0)
        copy = pltpu.make_async_copy(table, table_hbm, sem)
        copy.start()
        return copy

    for c in range(CHUNKS):

        def step(i, carry, c=c):
            output_rows(pl.multiple_of(c * rows + i * 8, 8))
            return carry

        lax.fori_loop(0, rows // 8, step, 0, unroll=True)
        part = pl.ds(c * rows, rows)
        group = [
            pltpu.make_async_copy(kin.at[part], kin_hbm.at[part], sem),
            pltpu.make_async_copy(rad.at[part], rad_hbm.at[part], sem),
        ]
        for copy in group:
            copy.start()
        stores += group
        if c == 1:
            stores.append(make_table())
    for copy in stores:
        copy.wait()


def scoped_output(halos, *refs):
    pl.run_scoped(
        lambda sem: output_kernel(halos, *refs, sem=sem), pltpu.SemaphoreType.DMA
    )


def solution(mesh):
    groups, domains = mesh.shape["grp"], mesh.shape["dom"]

    def local(
        positions, velocities, masses, block_halo, block_shift, block_live, block_count, home_slot
    ):
        blocks, width = masses.shape
        halos = home_slot.shape[0]
        owned = halos // (groups * domains)
        near = 3 * domains - 1
        far = (groups - 3) * domains
        vmem = pl.BlockSpec(memory_space=pltpu.VMEM)
        hbm = pl.BlockSpec(memory_space=pl.ANY)
        dma = pltpu.SemaphoreType.DMA
        pos, vel, means, sums, live = pl.pallas_call(
            functools.partial(scoped_exchange, groups, domains, owned, len(chunk_spans(blocks))),
            out_shape=(
                pltpu.VMEM((3, blocks, width), F32),
                pltpu.VMEM((3, blocks, width), F32),
                pltpu.VMEM((blocks, LANES), F32),
                pltpu.VMEM((16, owned), F32),
                pltpu.VMEM((blocks, LANES), F32),
            ),
            in_specs=[hbm] * 6 + [pl.BlockSpec(memory_space=pltpu.SMEM), hbm],
            out_specs=(vmem,) * 5,
            scratch_shapes=[
                pltpu.VMEM((1, blocks), jnp.int32),
                pltpu.VMEM((3, blocks), jnp.int32),
                pltpu.VMEM((1, blocks), jnp.int32),
                pltpu.VMEM((halos // LANES, LANES), jnp.int32),
                pltpu.VMEM((blocks, width), F32),
                pltpu.VMEM((blocks, LANES), F32),
                pltpu.VMEM((SUMS, blocks, LANES), F32),
                pltpu.VMEM((blocks, LANES), F32),
                pltpu.VMEM((16, blocks), F32),
                pltpu.VMEM((1, 1, blocks), F32),
                pltpu.VMEM((near, 16, blocks), F32),
                pltpu.VMEM((far, blocks), F32),
                dma((3,)),
            ],
            compiler_params=pltpu.CompilerParams(collective_id=0, has_side_effects=True),
        )(
            positions, velocities, masses,
            block_halo.reshape(1, blocks), block_shift, block_live.reshape(1, blocks),
            block_count, home_slot.reshape(halos // LANES, LANES),
        )
        return pl.pallas_call(
            functools.partial(scoped_output, halos),
            out_shape=(
                jax.ShapeDtypeStruct((11, owned), F32),
                jax.ShapeDtypeStruct((blocks, width), F32),
                jax.ShapeDtypeStruct((blocks, width), F32),
            ),
            in_specs=[vmem] * 5,
            out_specs=(hbm, hbm, hbm),
            scratch_shapes=[
                pltpu.VMEM((11, owned), F32),
                pltpu.VMEM((blocks, width), F32),
                pltpu.VMEM((blocks, width), F32),
            ],
        )(*[pltpu.with_memory_space_constraint(x, pltpu.VMEM) for x in (pos, vel, means, sums, live)])

    return jax.shard_map(
        local,
        mesh=mesh,
        in_specs=(
            P(None, ("grp", "dom"), None),
            P(None, ("grp", "dom"), None),
            P(("grp", "dom"), None),
            P(("grp", "dom")),
            P(None, ("grp", "dom")),
            P(("grp", "dom")),
            P(("grp", "dom")),
            P(),
        ),
        out_specs=(P(None, ("grp", "dom")), P(("grp", "dom"), None), P(("grp", "dom"), None)),
        check_vma=False,
    )
```

```python
import functools

import jax
import jax.numpy as jnp
from jax import lax
from jax.experimental import pallas as pl
from jax.experimental.pallas import tpu as pltpu
from jax.sharding import PartitionSpec as P

BOX = 1.0
EPSILON = 1e-06
MESH = pl.DeviceIdType.MESH
F32 = jnp.float32
BF16 = jnp.bfloat16
LANES = 128
CHUNKS = 4
SLOT_ROW = 8
SPIN_ROW = 9
USED_ROWS = 12
SUMS = 11
MASS_ROW = 12


def pieces(x):
    hi = x.astype(BF16).astype(F32)
    rest = x - hi
    mid = rest.astype(BF16).astype(F32)
    return hi, mid, rest - mid


def quotient(x, n):
    return x >> (n.bit_length() - 1) if n & (n - 1) == 0 else x // n


def crossed(a, b):
    return (a[1] * b[2] - a[2] * b[1], a[2] * b[0] - a[0] * b[2], a[0] * b[1] - a[1] * b[0])


def chunk_spans(blocks):
    tail = max(blocks // 8, 8)
    middle = max(3 * blocks // 8 // 8 * 8, 8)
    first = blocks - middle - tail
    return [(0, first), (first, middle), (first + middle, tail)]


def exchange_kernel(
    groups, domains, owned,
    pos_hbm, vel_hbm, mass_hbm, halo_hbm, shift_hbm, live_hbm, count_ref, home_hbm,
    pos, vel, means_ref, sums_ref, cols,
    halo_ref, shift_ref, live_ref, home_ref, mass, slots, partial, moments, tile, mass_row, near_in, far_in,
    recv_sem, small_sem=None, in_sem=None, tick=None,
):
    blocks, width = mass.shape
    spans = chunk_spans(blocks)
    g = lax.axis_index("grp")
    d = lax.axis_index("dom")

    def wrapped(x, n):
        return jnp.where(x >= n, x - n, x)

    def peer(dg, dd):
        return {"grp": wrapped(g + dg % groups, groups), "dom": wrapped(d + dd % domains, domains)}

    pairs = (
        (live_hbm, live_ref), (halo_hbm, halo_ref), (home_hbm, home_ref),
        (shift_hbm, shift_ref),
    )
    smalls = [
        pltpu.make_async_copy(src, dst, small_sem) for src, dst in pairs
    ]
    for copy in smalls:
        copy.start()
    turns = sorted(range(domains), key=lambda dd: -min(dd, domains - dd))
    ahead = [(1, dd) for dd in turns]
    behind = [(groups - 1, dd) for dd in turns]
    inside = [(0, dd) for dd in turns[:-1]]
    far = [(dg, dd) for dg in range(2, groups - 1) for dd in turns]
    near = ahead + behind + inside
    barrier = pltpu.get_barrier_semaphore()
    peers = near + far
    pl.semaphore_signal(tick, 1)
    loads = []
    for c, (start, rows) in enumerate(spans):
        part = pl.ds(start, rows)
        group = [
            pltpu.make_async_copy(mass_hbm.at[part], mass.at[part], in_sem.at[c]),
            pltpu.make_async_copy(pos_hbm.at[:, part], pos.at[:, part], in_sem.at[c]),
            pltpu.make_async_copy(vel_hbm.at[:, part], vel.at[:, part], in_sem.at[c]),
        ]
        for copy in group:
            copy.start(priority=1)
        loads.append(group)

    for dg, dd in peers:
        pl.semaphore_signal(barrier, inc=1, device_id=peer(dg, dd), device_id_type=MESH)
    pl.semaphore_wait(tick, 1)

    for copy in smalls:
        copy.wait()

    lane = lax.broadcasted_iota(jnp.int32, (blocks, LANES), 1)
    row = lax.broadcasted_iota(jnp.int32, (blocks, 1), 0)
    packed = jnp.concatenate(
        [
            halo_ref[...].astype(F32),
            live_ref[...].astype(F32),
            jnp.zeros((6, blocks), F32),
        ],
        axis=0,
    )
    turned = packed.T
    live_col = jnp.where(row < count_ref[0], turned[:, 1:2], 0.0)
    cols[...] = jnp.broadcast_to(live_col, (blocks, LANES))

    halo = turned[:, 0:1].astype(jnp.int32)
    home = home_ref[...]
    home_rows = home.shape[0]
    row_pick = lax.broadcasted_iota(jnp.int32, (blocks, home_rows), 1) == quotient(halo, LANES)
    split = jnp.concatenate([(home >> 8).astype(F32), (home & 255).astype(F32)], axis=1)
    picked = jnp.dot(
        row_pick.astype(F32).astype(BF16), split.astype(BF16), preferred_element_type=F32
    )
    value = picked[:, :LANES] * 256.0 + picked[:, LANES:]
    slot = jnp.sum(jnp.where(lane == (halo & (LANES - 1)), value, 0.0), axis=1, keepdims=True)
    slots[...] = jnp.broadcast_to(slot, (blocks, LANES))

    lane8 = lax.broadcasted_iota(jnp.int32, (8, LANES), 1)
    shift = shift_ref[...].astype(F32) * BOX

    def add_up(start):
        at = pl.ds(start, 8)
        live = cols[at]
        sums = None
        for t in range(width // LANES):
            span = pl.ds(t * LANES, LANES)
            place = (lane8 + t * LANES).astype(F32)
            w = jnp.where(place < live, mass[at, span], 0.0)
            x = [pos[k, at, span] for k in range(3)]
            v = [vel[k, at, span] for k in range(3)]
            wv = [w * y for y in v]
            made = [w] + [w * y for y in x] + wv
            made += [wv[0] * v[0] + wv[1] * v[1] + wv[2] * v[2]]
            made += list(crossed(x, wv))
            sums = made if sums is None else [a + b for a, b in zip(sums, made)]
        for k, y in enumerate(sums):
            partial[k, at] = y

    def fold(start):
        at = pl.ds(start, 8)
        out = jnp.where(lane8 == SLOT_ROW, slots[at], 0.0)
        for k in range(SUMS):
            lane_at = k if k < SLOT_ROW else k + 1
            out = jnp.where(lane8 == lane_at, jnp.sum(partial[k, at], axis=1, keepdims=True), out)
        moments[at] = out

    for c, (start, rows) in enumerate(spans):
        for copy in loads[c]:
            copy.wait()
        for i in range(start, start + rows, 8):
            add_up(i)
            fold(i)

    by_row = moments[...].T[:16]
    blank = jnp.zeros((1, blocks), F32)
    s = [shift[k:k + 1] for k in range(3)]
    v = [by_row[4 + k:5 + k] for k in range(3)]

    def stack(x, first):
        return jnp.concatenate([blank] * first + list(x) + [blank] * (5 - first), axis=0)

    first = by_row[0:8] + stack(s, 1) * by_row[0:1]
    turn = stack((s[1], s[2], s[0]), 1) * stack((v[2], v[0], v[1]), 1)
    turn = turn - stack((s[2], s[0], s[1]), 1) * stack((v[1], v[2], v[0]), 1)
    second = by_row[8:16] + turn
    tile[0:8] = first
    tile[8:16] = second
    mass_row[0] = first[0:1]

    pl.semaphore_wait(barrier, len(near) + len(far))

    def remote(src, dst, send, recv, dg, dd):
        return pltpu.make_async_remote_copy(
            src_ref=src, dst_ref=dst, send_sem=send, recv_sem=recv,
            device_id=peer(dg, dd), device_id_type=MESH,
        )

    used = pl.ds(0, USED_ROWS)
    from_behind, from_ahead, from_inside = 0, 1, 2
    send, send_far = in_sem.at[0], in_sem.at[1]
    late, early, recv_far = (recv_sem.at[k] for k in range(3))

    def send_near(first, last):
        for k in range(first, last):
            recv = late if k < domains else early
            remote(tile.at[used], near_in.at[k, used], send, recv, *near[k]).start()

    send_near(0, 2 * domains)
    for k, (dg, dd) in enumerate(far):
        remote(mass_row.at[0], far_in.at[pl.ds(k, 1)], send_far, recv_far, dg, dd).start()
    send_near(2 * domains, len(near))

    row8 = lax.broadcasted_iota(jnp.int32, (8, blocks), 0)
    base = ((g * domains + d) * owned).astype(F32)
    mine = lax.broadcasted_iota(jnp.int32, (owned, blocks), 0).astype(F32) + base

    def matched(rows, hits):
        left = jnp.concatenate(
            [jnp.concatenate(list(pieces(x)), axis=0) for x in rows], axis=1
        ).astype(BF16)
        right = jnp.concatenate([x.astype(F32) for x in hits], axis=1).astype(BF16)
        out = lax.dot_general(left, right, (((1,), (1,)), ((), ())), preferred_element_type=F32)
        n = rows[0].shape[0]
        return out[0:n] + out[n:2 * n] + out[2 * n:3 * n]

    def means_from(tiles):
        return matched([t[0] for t in tiles], [slots[...] == t[1][0:1] for t in tiles])

    def sums_from(tiles):
        kept = [jnp.where(row8 < USED_ROWS - 8, t[1], 0.0) for t in tiles]
        both = [jnp.concatenate([t[0], x], axis=0) for t, x in zip(tiles, kept)]
        return matched(both, [mine == t[1][0:1] for t in tiles])

    def landed(ref, recv):
        remote(ref, ref, send, recv, *near[0]).wait_recv()

    def inbox(k):
        at = range(k * domains, (k + 1) * domains if k < from_inside else len(near))
        return [(near_in[n, 0:8], near_in[n, 8:16]) for n in at]

    def masses_of(tiles):
        return functools.reduce(lambda a, b: a + b, [t[0][0:1] for t in tiles])

    landed(near_in.at[pl.ds(domains, len(near) - domains), used], early)
    if far:
        landed(far_in, recv_far)
    tiles = inbox(from_inside)
    total = first[0:1] + masses_of(tiles)
    means = means_from([(first, second)] + tiles)
    sums = sums_from([(first, second)] + tiles)
    tiles = inbox(from_ahead)
    total = total + masses_of(tiles)
    means = means + means_from(tiles)
    whole = near_in.at[:, used]
    remote(whole, whole, send, early, *near[0]).wait_send()
    if far:
        remote(far_in, far_in, send_far, recv_far, *near[0]).wait_send()
        total = total + jnp.sum(far_in[...], axis=0, keepdims=True)
    landed(near_in.at[pl.ds(0, domains), used], late)
    tiles = inbox(from_behind)
    total = total + masses_of(tiles)
    means = means + means_from(tiles)

    centre, drift, spread = halo_means(means)
    by_block = jnp.concatenate(
        [centre[k] - s[k] for k in range(3)]
        + drift
        + [1.0 / (3.0 * spread + EPSILON), blank],
        axis=0,
    )
    means_ref[:, 0:8] = by_block.T
    sums = sums + sums_from(tiles)
    sums_ref[0:8] = sums[0:8]
    sums_ref[8:16] = jnp.where(row8 == MASS_ROW - 8, total, sums[8:16])


def scoped_exchange(groups, domains, owned, chunks, *refs):
    dma = pltpu.SemaphoreType.DMA
    pl.run_scoped(
        lambda small_sem, in_sem, tick: exchange_kernel(
            groups, domains, owned, *refs, small_sem=small_sem, in_sem=in_sem, tick=tick
        ),
        dma, dma((chunks,)), pltpu.SemaphoreType.REGULAR,
    )


def halo_means(sums):
    scaled = sums[1:8] * (1.0 / jnp.maximum(sums[0:1], 1.0))
    centre = [scaled[k:k + 1] for k in range(3)]
    drift = [scaled[3 + k:4 + k] for k in range(3)]
    spread = scaled[6:7] - (drift[0] * drift[0] + drift[1] * drift[1] + drift[2] * drift[2])
    return centre, drift, spread


def output_kernel(
    halos, pos, vel, means_ref, sums_ref, live_ref, table_hbm, kin_hbm, rad_hbm, table, kin, rad, sem=None
):
    blocks, width = kin.shape
    rows = blocks // CHUNKS
    stores = []

    lane8 = lax.broadcasted_iota(jnp.int32, (8, LANES), 1)

    def output_rows(start):
        at = pl.ds(start, 8)
        mean = means_ref[at]
        mean = [jnp.broadcast_to(mean[:, k:k + 1], (8, LANES)) for k in range(7)]
        live = live_ref[at]
        for t in range(width // LANES):
            span = pl.ds(t * LANES, LANES)
            kinetic, radial = 0.0, 0.0
            for k in range(3):
                distance = pos[k, at, span] - mean[k]
                radial = radial + distance * distance
                offset = vel[k, at, span] - mean[3 + k]
                kinetic = kinetic + offset * offset
            kept = (lane8 + t * LANES).astype(F32) < live
            kin[at, span] = jnp.where(kept, kinetic * mean[6], 0.0)
            rad[at, span] = jnp.where(kept, radial, 0.0)

    def make_table():
        sums = sums_ref[...]
        centre, drift, spread = halo_means(sums)
        heavy_inv = 1.0 / jnp.maximum(sums[0:1], 1.0)
        turned_spin = crossed(centre, drift)
        spin = [sums[SPIN_ROW + k:SPIN_ROW + 1 + k] * heavy_inv - turned_spin[k] for k in range(3)]
        total = jnp.sum(sums[MASS_ROW:MASS_ROW + 1], axis=1, keepdims=True)
        share = sums[0:1] * float(halos) / total
        table[...] = jnp.concatenate([share] + centre + drift + [spread] + spin, axis=0)
        copy = pltpu.make_async_copy(table, table_hbm, sem)
        copy.start()
        return copy

    for c in range(CHUNKS):

        def step(i, carry, c=c):
            output_rows(pl.multiple_of(c * rows + i * 8, 8))
            return carry

        lax.fori_loop(0, rows // 8, step, 0, unroll=True)
        part = pl.ds(c * rows, rows)
        group = [
            pltpu.make_async_copy(kin.at[part], kin_hbm.at[part], sem),
            pltpu.make_async_copy(rad.at[part], rad_hbm.at[part], sem),
        ]
        for copy in group:
            copy.start()
        stores += group
        if c == 1:
            stores.append(make_table())
    for copy in stores:
        copy.wait()


def scoped_output(halos, *refs):
    pl.run_scoped(
        lambda sem: output_kernel(halos, *refs, sem=sem), pltpu.SemaphoreType.DMA
    )


def solution(mesh):
    groups, domains = mesh.shape["grp"], mesh.shape["dom"]

    def local(
        positions, velocities, masses, block_halo, block_shift, block_live, block_count, home_slot
    ):
        blocks, width = masses.shape
        halos = home_slot.shape[0]
        owned = halos // (groups * domains)
        near = 3 * domains - 1
        far = (groups - 3) * domains
        vmem = pl.BlockSpec(memory_space=pltpu.VMEM)
        hbm = pl.BlockSpec(memory_space=pl.ANY)
        dma = pltpu.SemaphoreType.DMA
        pos, vel, means, sums, live = pl.pallas_call(
            functools.partial(scoped_exchange, groups, domains, owned, len(chunk_spans(blocks))),
            out_shape=(
                pltpu.VMEM((3, blocks, width), F32),
                pltpu.VMEM((3, blocks, width), F32),
                pltpu.VMEM((blocks, LANES), F32),
                pltpu.VMEM((16, owned), F32),
                pltpu.VMEM((blocks, LANES), F32),
            ),
            in_specs=[hbm] * 6 + [pl.BlockSpec(memory_space=pltpu.SMEM), hbm],
            out_specs=(vmem,) * 5,
            scratch_shapes=[
                pltpu.VMEM((1, blocks), jnp.int32),
                pltpu.VMEM((3, blocks), jnp.int32),
                pltpu.VMEM((1, blocks), jnp.int32),
                pltpu.VMEM((halos // LANES, LANES), jnp.int32),
                pltpu.VMEM((blocks, width), F32),
                pltpu.VMEM((blocks, LANES), F32),
                pltpu.VMEM((SUMS, blocks, LANES), F32),
                pltpu.VMEM((blocks, LANES), F32),
                pltpu.VMEM((16, blocks), F32),
                pltpu.VMEM((1, 1, blocks), F32),
                pltpu.VMEM((near, 16, blocks), F32),
                pltpu.VMEM((far, blocks), F32),
                dma((3,)),
            ],
            compiler_params=pltpu.CompilerParams(collective_id=0, has_side_effects=True),
        )(
            positions, velocities, masses,
            block_halo.reshape(1, blocks), block_shift, block_live.reshape(1, blocks),
            block_count, home_slot.reshape(halos // LANES, LANES),
        )
        return pl.pallas_call(
            functools.partial(scoped_output, halos),
            out_shape=(
                jax.ShapeDtypeStruct((11, owned), F32),
                jax.ShapeDtypeStruct((blocks, width), F32),
                jax.ShapeDtypeStruct((blocks, width), F32),
            ),
            in_specs=[vmem] * 5,
            out_specs=(hbm, hbm, hbm),
            scratch_shapes=[
                pltpu.VMEM((11, owned), F32),
                pltpu.VMEM((blocks, width), F32),
                pltpu.VMEM((blocks, width), F32),
            ],
        )(*[pltpu.with_memory_space_constraint(x, pltpu.VMEM) for x in (pos, vel, means, sums, live)])

    return jax.shard_map(
        local,
        mesh=mesh,
        in_specs=(
            P(None, ("grp", "dom"), None),
            P(None, ("grp", "dom"), None),
            P(("grp", "dom"), None),
            P(("grp", "dom")),
            P(None, ("grp", "dom")),
            P(("grp", "dom")),
            P(("grp", "dom")),
            P(),
        ),
        out_specs=(P(None, ("grp", "dom")), P(("grp", "dom"), None), P(("grp", "dom"), None)),
        check_vma=False,
    )
```
